256 devices in a mesh: seq: 32 (over x, y, core), head: 8 (over z).
Axes of the slice: x: 4, y: 4, z: 8, core: 2. Of those that a mesh axis runs over, the one named last changes fastest.
Arguments:
- queries: bfloat16 [8192, 16, 128], P('seq', 'head'), may hold values from -30 to 30
- keys: bfloat16 [8192, 16, 128], P('seq', 'head'), may hold values from -12 to 12
- values: bfloat16 [8192, 16, 128], P('seq', 'head'), may hold values from -6 to 6
- log_forget: float32 [16, 8192], P('head', 'seq'), may hold values from -1.6 to 0
- strength: float32 [16, 8192], P('head', 'seq'), may hold values from 0.05 to 1
- out_weight: bfloat16 [2048, 2048], P('head'), may hold values from -0.125 to 0.125
Outputs:
- mixed: bfloat16 [8192, 2048], P(('seq', 'head'))
The draws below stay inside these ranges and needn't reach their ends.
All inputs are finite; a program needn't handle non-finite values.
Results may differ from the reference program's by a relative error of at most 0.018.
Values may be sent and summed in bfloat16 or wider, within the bound.
No kernel may reach another device: no remote copies, remote signals or barrier semaphores. Data moves between devices by JAX's collectives and lax.ppermute only.
A program may use at most 64 MiB of HBM per device.

```python
import math
import jax
import jax.numpy as jnp
from jax import lax

D = 2048
HEADS = 16
E = 128
WINDOW = 1024
CG_STEPS = 6
SEQUENCE_TOKENS = 8192


def paired(key):
    drawn_keys = jnp.clip(jax.random.normal(jax.random.fold_in(key, 101), (SEQUENCE_TOKENS, HEADS, E), jnp.float32), -6.0, 6.0)
    drawn_queries = jnp.clip(jax.random.normal(jax.random.fold_in(key, 102), (SEQUENCE_TOKENS, HEADS, E), jnp.float32), -6.0, 6.0)
    return (drawn_queries, drawn_keys)


def draw_queries(key, part):
    return paired(key)[0].astype(jnp.bfloat16)


def draw_keys(key, part):
    return paired(key)[1].astype(jnp.bfloat16)


def draw_log_forget(key, part):
    fast = jax.random.randint(jax.random.fold_in(key, 201), (HEADS,), 0, 2) == 1
    fast_rate = 1.0 / 40.0 * jnp.exp(jax.random.uniform(jax.random.fold_in(key, 202), (HEADS,), jnp.float32, -0.29, 0.29))
    slow_rate = 0.25 / SEQUENCE_TOKENS * jnp.exp(jax.random.uniform(jax.random.fold_in(key, 203), (HEADS,), jnp.float32, -0.7, 0.7))
    learning_rate = jnp.where(fast, fast_rate, slow_rate)[:, None]
    coarse_estimate = jax.random.uniform(jax.random.fold_in(key, 204), (HEADS, SEQUENCE_TOKENS), jnp.float32, 0.5, 1.5)
    table = jnp.exp(jax.random.uniform(jax.random.fold_in(key, 205), (SEQUENCE_TOKENS // 64 + 1,), jnp.float32, -0.7, 0.7))
    block_multiplier = table[jnp.arange(SEQUENCE_TOKENS) // 64]
    spike_position = jax.random.randint(jax.random.fold_in(key, 206), (2,), 0, SEQUENCE_TOKENS)
    training_loss = jax.random.uniform(jax.random.fold_in(key, 207), (HEADS, 2), jnp.float32, 0.2, 0.5)
    match_count = (jnp.arange(SEQUENCE_TOKENS)[None, :] == spike_position[:, None]).astype(jnp.float32)
    spike_events = jnp.dot(jnp.log1p(-training_loss), match_count)
    return -learning_rate * coarse_estimate * block_multiplier[None, :] + spike_events


def shard_levels(key, dims, pieces, least, high):
    level = 1.0
    for dim, shards_of in pieces:
        draws = jax.random.uniform(jax.random.fold_in(jax.random.fold_in(key, 6), dim), (shards_of,), jnp.float32, least / len(pieces), high / len(pieces))
        level = level * jnp.repeat(jnp.exp(draws), dims[dim] // shards_of).reshape((-1,) + (1,) * (len(dims) - 1 - dim))
    return level


def centred(key, extent, scale, bound, pieces=(), kind=jnp.bfloat16):
    factor_of = shard_levels(key, extent, pieces, -0.22, 0.18) if pieces else 1.0
    result = jax.random.normal(key, extent, jnp.float32) * scale * factor_of
    return jnp.minimum(jnp.maximum(result, -bound), bound).astype(kind)


def setup_inputs(seed: int = 0) -> dict:
    key_of = jax.random.split(jax.random.key(seed), 7)
    return {
        "queries": draw_queries(jax.random.fold_in(key_of[6], 71), 0),
        "keys": draw_keys(jax.random.fold_in(key_of[6], 71), 0),
        "values": centred(key_of[2], (SEQUENCE_TOKENS, HEADS, E), 1.0, 6.0, ((0, 32), (1, 8))),
        "log_forget": draw_log_forget(jax.random.fold_in(key_of[6], 71), 0),
        "strength": jnp.clip(jnp.exp(math.log(1.0) - 2.9957323 * jax.random.uniform(key_of[4], (HEADS, SEQUENCE_TOKENS), jnp.float32) ** shard_levels(key_of[4], (HEADS, SEQUENCE_TOKENS), ((0, 8), (1, 32)), -0.2, 0.2)), 0.05, 1.0),
        "out_weight": centred(key_of[5], (HEADS * E, D), (HEADS * E) ** -0.5, 0.125, ((0, 8),)),
    }


ridge = 0.25
highest = lax.Precision.HIGHEST
tiny_floor = 1e-30

def window_attention(query_rows, key_rows, value_rows, offset):
    count = query_rows.shape[0]
    block = min(512, count)
    reach = WINDOW + block
    scale = query_rows.shape[2] ** (-0.5)
    results = []
    for block_start in range(0, count, block):
        query_block = query_rows[block_start:block_start + block].astype(jnp.float32)
        key_block = key_rows[block_start:block_start + reach].astype(jnp.float32)
        value_block = value_rows[block_start:block_start + reach].astype(jnp.float32)
        query_pos = block_start + jnp.arange(block)
        key_pos = block_start - WINDOW + jnp.arange(reach)
        admitted = (key_pos[None, :] <= query_pos[:, None]) & (key_pos[None, :] > query_pos[:, None] - WINDOW) & (key_pos[None, :] + offset >= 0)
        scores = jnp.einsum('qhe,khe->hqk', query_block, key_block, precision=highest) * scale
        scores = jnp.where(admitted[None], scores, -jnp.inf)
        largest = lax.optimization_barrier(jnp.max(scores, axis=-1, keepdims=True))
        expo = jnp.exp(scores - largest)
        weights = (expo / lax.optimization_barrier(jnp.sum(expo, axis=-1, keepdims=True))).astype(jnp.bfloat16)
        results.append(jnp.einsum('hqk,khe->qhe', weights.astype(jnp.float32), value_block, precision=highest))
    return jnp.concatenate(results, axis=0)

def group_step(state, inputs):
    key_state, value_state = state
    query_part, key_part, value_part, forget_part, strength_part = inputs
    decay_sum = jnp.cumsum(forget_part, axis=1)
    length = forget_part.shape[1]
    order = jnp.arange(length)
    causal = (order[:, None] >= order[None, :])[None]
    gap = jnp.where(causal, decay_sum[:, :, None] - decay_sum[:, None, :], 0.0)
    mixing = jnp.where(causal, jnp.exp(gap), 0.0) * strength_part[:, None, :]
    leading = jnp.exp(decay_sum)[:, :, None]

    def operator(vector):
        correlation = jnp.einsum('htf,hsf->hts', vector, key_part, precision=highest)
        carried = jnp.einsum('htf,hef->hte', vector, key_state, precision=highest)
        inside = jnp.einsum('hts,hse->hte', mixing * correlation, key_part, precision=highest)
        return leading * carried + inside + ridge * vector
    solution = jnp.zeros_like(query_part)
    residual = query_part
    direction = query_part
    norm_now = lax.optimization_barrier(jnp.sum(residual * residual, axis=-1, keepdims=True))
    for iteration in range(CG_STEPS):
        image = operator(direction)
        alpha = norm_now / jnp.maximum(lax.optimization_barrier(jnp.sum(direction * image, axis=-1, keepdims=True)), tiny_floor)
        solution = solution + alpha * direction
        residual = residual - alpha * image
        norm_next = lax.optimization_barrier(jnp.sum(residual * residual, axis=-1, keepdims=True))
        direction = residual + norm_next / jnp.maximum(norm_now, tiny_floor) * direction
        norm_now = norm_next
    correlation = jnp.einsum('htf,hsf->hts', solution, key_part, precision=highest)
    output = leading * jnp.einsum('htf,hef->hte', solution, value_state, precision=highest)
    output = output + jnp.einsum('hts,hse->hte', mixing * correlation, value_part, precision=highest)
    tail = jnp.exp(decay_sum[:, -1:] - decay_sum) * strength_part
    end_factor = jnp.exp(decay_sum[:, -1])[:, None, None]
    key_state = end_factor * key_state + jnp.einsum('hse,hsf->hef', tail[:, :, None] * key_part, key_part, precision=highest)
    value_state = end_factor * value_state + jnp.einsum('hse,hsf->hef', tail[:, :, None] * value_part, key_part, precision=highest)
    return ((key_state, value_state), output)

def normalized(rows):
    wide = rows.astype(jnp.float32)
    return wide * lax.rsqrt(lax.optimization_barrier(jnp.sum(wide * wide, axis=-1, keepdims=True)) + 1e-06)

def mesa_heads(query_rows, key_rows, value_rows, log_forget, strength, key_start, value_start):
    heads_here, count, width = query_rows.shape
    group = min(256, count)
    blocks = count // group

    def blocked(array):
        shaped = array.reshape((heads_here, blocks, group) + array.shape[2:])
        return jnp.moveaxis(shaped, 1, 0)
    inputs = (blocked(query_rows), blocked(key_rows), blocked(value_rows), blocked(log_forget), blocked(strength))
    final, outputs = lax.scan(group_step, (key_start, value_start), inputs)
    return jnp.moveaxis(outputs, 0, 1).reshape(heads_here, count, width)

def reference(queries, keys, values, log_forget, strength, out_weight):
    padding = jnp.zeros((WINDOW, HEADS, E), jnp.bfloat16)
    attended = window_attention(queries, jnp.concatenate((padding, keys), 0), jnp.concatenate((padding, values), 0), 0)
    query_norm = jnp.transpose(normalized(queries), (1, 0, 2))
    key_norm = jnp.transpose(normalized(keys), (1, 0, 2))
    value_wide = jnp.transpose(values.astype(jnp.float32), (1, 0, 2))
    empty = jnp.zeros((HEADS, E, E), jnp.float32)
    mesa = mesa_heads(query_norm, key_norm, value_wide, log_forget, strength, empty, empty)
    head_out = (attended + jnp.transpose(mesa, (1, 0, 2))).astype(jnp.bfloat16)
    flat = head_out.reshape(SEQUENCE_TOKENS, HEADS * E)
    return jnp.dot(flat, out_weight, preferred_element_type=jnp.float32).astype(jnp.bfloat16)
```

```python
import jax
import jax.numpy as jnp
from jax import lax
from jax.experimental import pallas as pl
from jax.experimental.pallas import tpu as pltpu
from jax.sharding import Mesh
from jax.sharding import PartitionSpec as P

WINDOW = 1024
CG_STEPS = 6
RIDGE = 0.25
TINY = 1e-30
LOW = -1e30
HALF = 256
E = 128
CHIP = 2 * HALF
ROWS = 2 * E + 16
SEQ = ("x", "y", "c")
XY = ("x", "y")
f32 = jnp.float32
bf16 = jnp.bfloat16


def spec(kind=pltpu.VMEM):
    return pl.BlockSpec(memory_space=kind)


def call(body, outs, scratch, flops, *args):
    return pl.pallas_call(
        body,
        out_shape=[jax.ShapeDtypeStruct(shape, kind) for shape, kind in outs],
        in_specs=[spec(pltpu.SMEM)] + [spec()] * (len(args) - 1),
        out_specs=[spec()] * len(outs),
        scratch_shapes=[pltpu.VMEM(shape, kind) for shape, kind in scratch],
        cost_estimate=pl.CostEstimate(flops=flops, bytes_accessed=1 << 20, transcendentals=0),
    )(*args)


def split(x):
    high = x.astype(bf16)
    return high, (x - high.astype(f32)).astype(bf16)


def dot(a, b):
    return jnp.dot(a, b, preferred_element_type=f32)


def two_part(a, b):
    high, low = split(b)
    return dot(a, high) + dot(a, low)


def iotas(shape):
    return lax.broadcasted_iota(jnp.int32, shape, 0), lax.broadcasted_iota(jnp.int32, shape, 1)


def payload(state, total):
    high, low = split(total)
    row, _ = iotas((16, E))
    tail = jnp.where(row == 0, high.astype(f32), jnp.where(row == 1, low.astype(f32), 0.0))
    return jnp.concatenate((state, tail), axis=0).astype(bf16)


def decay_row(tail):
    wide = tail.astype(f32)
    return wide[0:1, :] + wide[1:2, :]


def gram_body(pos, keep, recv, gate_keep, gate_recv, q_out, kv_out, gates_out, pay_out, first_out):
    core = pos[0]
    for source, which in ((keep, core), (recv, 1 - core)):
        rows = pl.ds(pl.multiple_of(which * HALF, HALF), HALF)
        q_out[rows, :] = source[0]
        kv_out[0, rows, :] = source[1]
        kv_out[1, rows, :] = source[2]
    a, b = gate_keep[...], gate_recv[...]
    first, second = jnp.where(core == 0, a, b), jnp.where(core == 0, b, a)
    forget = jnp.concatenate((first[0:1], second[0:1], jnp.zeros((6, HALF), f32)), axis=0)
    row, col = iotas((HALF, HALF))
    upto = (row <= col).astype(f32)
    sums = jnp.dot(forget, upto, preferred_element_type=f32, precision=lax.Precision.HIGHEST)
    gates_out[...] = jnp.concatenate(
        (sums[0:2], first[1:2], second[1:2], jnp.zeros((4, HALF), f32)), axis=0
    )
    grams = []
    for j in range(2):
        own = slice(j * HALF, (j + 1) * HALF)
        k = kv_out[0, own, :]
        kt = jnp.transpose(k.astype(f32))
        vt = jnp.transpose(kv_out[1, own, :].astype(f32))
        r = lax.rsqrt(jnp.sum(kt * kt, axis=0, keepdims=True) + 1e-6)
        weight = jnp.exp(sums[j : j + 1, HALF - 1 :] - sums[j : j + 1]) * gates_out[2 + j : 3 + j]
        left = jnp.concatenate((kt * (weight * r * r), vt * (weight * r)), axis=0)
        high, low = split(left)
        grams.append(dot(high, k) + dot(low, k))
    first_out[...] = grams[0]
    later = sums[1:2, HALF - 1 :]
    local = jnp.exp(later) * grams[0] + grams[1]
    pay_out[...] = payload(local, jnp.broadcast_to(sums[0:1, HALF - 1 :] + later, (1, E)))


def row_body(pos, own, r1, r2, r3, pay_out, state_out, lead_out, place):
    mine = pos[2]
    place[mine] = own[...]
    for distance, received in ((1, r1), (2, r2), (3, r3)):
        place[lax.rem(mine + 4 - distance, 4)] = received[...]
    decays = [decay_row(place[m, 2 * E :, :]) for m in range(4)]
    zero = jnp.zeros((1, E), f32)
    total = before = jnp.zeros((2 * E, E), f32)
    lead = zero
    for m in range(4):
        block = place[m, : 2 * E, :].astype(f32)
        step = jnp.exp(decays[m])
        total = step * total + block
        earlier = m < mine
        before = jnp.where(earlier, step * before + block, before)
        lead = jnp.where(earlier, lead + decays[m], lead)
    pay_out[...] = payload(total, decays[0] + decays[1] + decays[2] + decays[3])
    state_out[...] = before
    lead_out[...] = jnp.broadcast_to(lead, (8, E))


def solve_body(
    pos, q, kv, gates, first, state, lead, t1, t2, t3, out, left, keys_t, mix, mix_v, xs, rs, ds, rr
):
    line = pos[1]
    start = jnp.zeros((2 * E, E), f32)
    passed = jnp.zeros((1, E), f32)
    for distance, received in ((1, t1), (2, t2), (3, t3)):
        block = received[: 2 * E, :].astype(f32)
        start = jnp.where(line >= distance, start + jnp.exp(passed) * block, start)
        passed = passed + decay_row(received[2 * E :, :])
    start = jnp.exp(lead[0:1, :]) * start + state[...]
    starts = [start, jnp.exp(gates[0:1, HALF - 1 :]) * start + first[...]]
    row, col = iotas((HALF, HALF))
    causal = row <= col
    leads = []
    for j in range(2):
        own = slice(j * HALF, (j + 1) * HALF)
        k = kv[0, own, :]
        kt = jnp.transpose(k.astype(f32))
        keys_t[j] = kt.astype(bf16)
        r = lax.rsqrt(jnp.sum(kt * kt, axis=0, keepdims=True) + 1e-6)
        c = gates[j : j + 1, :]
        strength = gates[2 + j : 3 + j, :]
        line_of, _ = iotas((E, HALF))
        columns = jnp.transpose(
            jnp.where(
                line_of == 0, c, jnp.where(line_of == 1, strength * r * r, strength * r)
            )
        )
        gap = jnp.where(causal, c - columns[:, 0:1], 0.0)
        decay = jnp.where(causal, jnp.exp(gap), 0.0)
        mix[j] = decay * columns[:, 1:2]
        mix_v[j] = decay * columns[:, 2:3]
        leads.append(jnp.exp(c))
        left[j, :HALF, :E] = k
        left[j, :HALF, E:] = k
        high, low = split(starts[j][:E])
        left[j, HALF : HALF + E, :E] = high
        left[j, HALF : HALF + E, E:] = high
        left[j, HALF + E :, :E] = low
        left[j, HALF + E :, E:] = jnp.zeros((E, E), bf16)
        qt = jnp.transpose(q[own, :].astype(f32))
        qn = qt * lax.rsqrt(jnp.sum(qt * qt, axis=0, keepdims=True) + 1e-6)
        xs[j] = jnp.zeros((E, HALF), f32)
        rs[j] = qn
        ds[j] = qn
        rr[j] = jnp.sum(qn * qn, axis=0, keepdims=True)

    def products(j, vector, weights, right):
        high, low = split(vector)
        y = dot(left[j], jnp.concatenate((high, low), axis=0))
        inside = two_part(right, weights * y[:HALF])
        return leads[j] * (y[HALF : HALF + E] + y[HALF + E :]) + inside

    def iteration(_, carry):
        for j in range(2):
            d = ds[j]
            image = products(j, d, mix[j], keys_t[j]) + RIDGE * d
            now = rr[j]
            alpha = now / jnp.maximum(jnp.sum(d * image, axis=0, keepdims=True), TINY)
            xs[j] = xs[j] + alpha * d
            r = rs[j] - alpha * image
            rs[j] = r
            new = jnp.sum(r * r, axis=0, keepdims=True)
            ds[j] = r + new / jnp.maximum(now, TINY) * d
            rr[j] = new
        return carry

    lax.fori_loop(0, CG_STEPS, iteration, 0)
    for j in range(2):
        own = slice(j * HALF, (j + 1) * HALF)
        high, low = split(starts[j][E:])
        left[j, HALF : HALF + E, :E] = high
        left[j, HALF : HALF + E, E:] = high
        left[j, HALF + E :, :E] = low
        vt = jnp.transpose(kv[1, own, :].astype(f32)).astype(bf16)
        out[:, own] = products(j, xs[j], mix_v[j], vt)


def attend_body(pos, q, kv, near, far, mesa, keep_out, send_out):
    core, chip = pos[0], pos[1] * 4 + pos[2]
    scale = E ** (-0.5)
    row, col = iotas((HALF, HALF))
    parts = [(far, 0, 2), (far, 1, 2), (near, 0, 1), (near, 1, 1), (kv, 0, 0), (kv, 1, 0)]

    def rows_of(b, which):
        source, half, _ = parts[b]
        return source[which, half * HALF : (half + 1) * HALF, :]

    values_t = [jnp.transpose(rows_of(b, 1).astype(f32)).astype(bf16) for b in range(6)]
    for j in range(2):
        own = slice(j * HALF, (j + 1) * HALF)
        qj = q[own, :]
        scores = []
        for b in range(j, j + 5):
            s = lax.dot_general(
                rows_of(b, 0), qj, (((1,), (1,)), ((), ())), preferred_element_type=f32
            )
            if b == j:
                s = jnp.where(row > col, s, LOW)
            if b == j + 4:
                s = jnp.where(row <= col, s, LOW)
            if parts[b][2]:
                s = jnp.where(chip >= parts[b][2], s, LOW)
            scores.append(s)
        largest = scores[0]
        for s in scores[1:]:
            largest = jnp.maximum(largest, s)
        largest = jnp.max(largest, axis=0, keepdims=True)
        total = jnp.zeros((1, HALF), f32)
        result = jnp.zeros((E, HALF), f32)
        for b, s in zip(range(j, j + 5), scores):
            expo = jnp.exp((s - largest) * scale)
            total = total + jnp.sum(expo, axis=0, keepdims=True)
            result = result + dot(values_t[b], expo.astype(bf16))
        both = jnp.transpose(result / total + mesa[:, own]).astype(bf16)

        @pl.when(core == j)
        def _():
            keep_out[...] = both

        @pl.when(core != j)
        def _():
            send_out[...] = both


def swapped(x):
    return lax.ppermute(x, "c", [(0, 1), (1, 0)])


def turned(x, axis, by):
    return lax.ppermute(x, axis, [(i, (i + by) % 4) for i in range(4)])


def on_device(queries, keys, values, log_forget, strength, out_weight):
    core, x, y = (lax.axis_index(a) for a in ("c", "x", "y"))
    pos = jnp.stack((core, x, y)).astype(jnp.int32)
    rows = jnp.stack((queries, keys, values))
    gates = jnp.stack((log_forget, strength), axis=1)
    front = core == 0
    keep = jnp.where(front, rows[:, :, 0], rows[:, :, 1])
    send = jnp.where(front, rows[:, :, 1], rows[:, :, 0])
    gate_keep = jnp.where(front, gates[0], gates[1])
    gate_send = jnp.where(front, gates[1], gates[0])
    q, kv, gates, local, first = call(
        gram_body,
        [
            ((CHIP, E), bf16),
            ((2, CHIP, E), bf16),
            ((8, HALF), f32),
            ((ROWS, E), bf16),
            ((2 * E, E), f32),
        ],
        [],
        1 << 26,
        pos,
        keep,
        swapped(send),
        gate_keep,
        swapped(gate_send),
    )
    near, far = (
        lax.ppermute(kv, XY, [(i, i + by) for i in range(16) if i + by < 16]) for by in (1, 2)
    )
    row_total, state, lead = call(
        row_body,
        [((ROWS, E), bf16), ((2 * E, E), f32), ((8, E), f32)],
        [((4, ROWS, E), bf16)],
        1 << 20,
        pos,
        local,
        *(turned(local, "y", by) for by in (1, 2, 3)),
    )
    (mesa,) = call(
        solve_body,
        [((E, CHIP), f32)],
        [
            ((2, CHIP, CHIP // 2), bf16),
            ((2, E, HALF), bf16),
            ((2, HALF, HALF), f32),
            ((2, HALF, HALF), f32),
            ((2, E, HALF), f32),
            ((2, E, HALF), f32),
            ((2, E, HALF), f32),
            ((2, 1, HALF), f32),
        ],
        1 << 30,
        pos,
        q,
        kv,
        gates,
        first,
        state,
        lead,
        *(turned(row_total, "x", by) for by in (1, 2, 3)),
    )
    kept, sent = call(
        attend_body, [((HALF, E), bf16)] * 2, [], 1 << 29, pos, q, kv, near, far, mesa
    )
    other = swapped(sent)
    flat = jnp.concatenate(
        (jnp.where(front, kept, other), jnp.where(front, other, kept)), axis=1
    )
    shares = jnp.dot(flat, out_weight, preferred_element_type=f32).astype(bf16)
    parts = lax.all_to_all(shares.reshape(8, 32, 2048), "z", 0, 0, tiled=True)
    return jnp.sum(parts.astype(f32), axis=0).astype(bf16)


def solution(mesh):
    grid = Mesh(mesh.devices.reshape(4, 4, 2, mesh.shape["head"]), ("x", "y", "c", "z"))
    in_specs = (
        P(SEQ, "z", None),
        P(SEQ, "z", None),
        P(SEQ, "z", None),
        P("z", SEQ),
        P("z", SEQ),
        P("z", None),
    )
    return jax.shard_map(
        on_device, mesh=grid, in_specs=in_specs, out_specs=P((*SEQ, "z"), None), check_vma=False
    )
```

```python
import jax
import jax.numpy as jnp
from jax import lax
from jax.experimental import pallas as pl
from jax.experimental.pallas import tpu as pltpu
from jax.sharding import Mesh
from jax.sharding import PartitionSpec as P

CG_STEPS = 6
RIDGE = 0.25
TINY = 1e-30
LOW = -1e30
HALF = 256
E = 128
CHIP = 2 * HALF
ROWS = 2 * E + 16
SLOT = 32
GRANT = 16 << 20
SEQ = ("x", "y", "c")
XY = ("x", "y")
f32 = jnp.float32
bf16 = jnp.bfloat16


def spec(kind=pltpu.VMEM):
    return pl.BlockSpec(memory_space=kind)


def call(body, outs, scratch, flops, *args):
    return pl.pallas_call(
        body,
        out_shape=[jax.ShapeDtypeStruct(shape, kind) for shape, kind in outs],
        in_specs=[spec(pltpu.SMEM)] + [spec()] * (len(args) - 1),
        out_specs=[spec()] * len(outs),
        scratch_shapes=[pltpu.VMEM(shape, kind) for shape, kind in scratch],
        compiler_params=pltpu.CompilerParams(vmem_limit_bytes=GRANT),
        cost_estimate=pl.CostEstimate(flops=flops, bytes_accessed=1 << 20, transcendentals=0),
    )(*args)


def split(x):
    high = x.astype(bf16)
    return high, (x - high.astype(f32)).astype(bf16)


def dot(a, b):
    return jnp.dot(a, b, preferred_element_type=f32)


def two_part(a, b):
    high, low = split(b)
    return dot(a, high) + dot(a, low)


def iotas(shape):
    return lax.broadcasted_iota(jnp.int32, shape, 0), lax.broadcasted_iota(jnp.int32, shape, 1)


def payload(state, total):
    high, low = split(total)
    row, _ = iotas((16, E))
    tail = jnp.where(row == 0, high.astype(f32), jnp.where(row == 1, low.astype(f32), 0.0))
    return jnp.concatenate((state, tail), axis=0).astype(bf16)


def decay_row(tail):
    wide = tail.astype(f32)
    return wide[0:1, :] + wide[1:2, :]


def gram_body(pos, keep, recv, gate_keep, gate_recv, q_out, kv_out, gates_out, pay_out, first_out):
    core = pos[0]
    for source, which in ((keep, core), (recv, 1 - core)):
        rows = pl.ds(pl.multiple_of(which * HALF, HALF), HALF)
        q_out[rows, :] = source[0]
        kv_out[0, rows, :] = source[1]
        kv_out[1, rows, :] = source[2]
    a, b = gate_keep[...], gate_recv[...]
    first, second = jnp.where(core == 0, a, b), jnp.where(core == 0, b, a)
    forget = jnp.concatenate((first[0:1], second[0:1], jnp.zeros((6, HALF), f32)), axis=0)
    row, col = iotas((HALF, HALF))
    upto = (row <= col).astype(f32)
    sums = jnp.dot(forget, upto, preferred_element_type=f32, precision=lax.Precision.HIGHEST)
    gates_out[...] = jnp.concatenate(
        (sums[0:2], first[1:2], second[1:2], jnp.zeros((4, HALF), f32)), axis=0
    )
    grams = []
    for j in range(2):
        own = slice(j * HALF, (j + 1) * HALF)
        k = kv_out[0, own, :]
        kt = jnp.transpose(k.astype(f32))
        vt = jnp.transpose(kv_out[1, own, :].astype(f32))
        r = lax.rsqrt(jnp.sum(kt * kt, axis=0, keepdims=True) + 1e-6)
        weight = jnp.exp(sums[j : j + 1, HALF - 1 :] - sums[j : j + 1]) * gates_out[2 + j : 3 + j]
        left = jnp.concatenate((kt * (weight * r * r), vt * (weight * r)), axis=0)
        high, low = split(left)
        grams.append(dot(high, k) + dot(low, k))
    first_out[...] = grams[0]
    later = sums[1:2, HALF - 1 :]
    local = jnp.exp(later) * grams[0] + grams[1]
    pay_out[...] = payload(local, jnp.broadcast_to(sums[0:1, HALF - 1 :] + later, (1, E)))


def row_body(pos, own, r1, r2, r3, pay_out, state_out, lead_out, place):
    mine = pos[2]
    place[mine] = own[...]
    for distance, received in ((1, r1), (2, r2), (3, r3)):
        place[lax.rem(mine + 4 - distance, 4)] = received[...]
    decays = [decay_row(place[m, 2 * E :, :]) for m in range(4)]
    zero = jnp.zeros((1, E), f32)
    total = before = jnp.zeros((2 * E, E), f32)
    lead = zero
    for m in range(4):
        block = place[m, : 2 * E, :].astype(f32)
        step = jnp.exp(decays[m])
        total = step * total + block
        earlier = m < mine
        before = jnp.where(earlier, step * before + block, before)
        lead = jnp.where(earlier, lead + decays[m], lead)
    pay_out[...] = payload(total, decays[0] + decays[1] + decays[2] + decays[3])
    state_out[...] = before
    lead_out[...] = jnp.broadcast_to(lead, (8, E))


def solve_body(
    pos, q, kv, gates, first, state, lead, t1, t2, t3, out, left, keys_t, mix, mix_v, xs, rs, ds, rr
):
    line = pos[1]
    start = jnp.zeros((2 * E, E), f32)
    passed = jnp.zeros((1, E), f32)
    for distance, received in ((1, t1), (2, t2), (3, t3)):
        block = received[: 2 * E, :].astype(f32)
        start = jnp.where(line >= distance, start + jnp.exp(passed) * block, start)
        passed = passed + decay_row(received[2 * E :, :])
    start = jnp.exp(lead[0:1, :]) * start + state[...]
    starts = [start, jnp.exp(gates[0:1, HALF - 1 :]) * start + first[...]]
    row, col = iotas((HALF, HALF))
    causal = row <= col
    leads = []
    for j in range(2):
        own = slice(j * HALF, (j + 1) * HALF)
        k = kv[0, own, :]
        kt = jnp.transpose(k.astype(f32))
        keys_t[j] = kt.astype(bf16)
        r = lax.rsqrt(jnp.sum(kt * kt, axis=0, keepdims=True) + 1e-6)
        c = gates[j : j + 1, :]
        strength = gates[2 + j : 3 + j, :]
        line_of, _ = iotas((E, HALF))
        columns = jnp.transpose(
            jnp.where(
                line_of == 0, c, jnp.where(line_of == 1, strength * r * r, strength * r)
            )
        )
        gap = jnp.where(causal, c - columns[:, 0:1], 0.0)
        decay = jnp.where(causal, jnp.exp(gap), 0.0)
        mix[j] = decay * columns[:, 1:2]
        mix_v[j] = decay * columns[:, 2:3]
        leads.append(jnp.exp(c))
        left[j, :HALF, :E] = k
        left[j, :HALF, E:] = k
        high, low = split(starts[j][:E])
        left[j, HALF : HALF + E, :E] = high
        left[j, HALF : HALF + E, E:] = high
        left[j, HALF + E :, :E] = low
        left[j, HALF + E :, E:] = jnp.zeros((E, E), bf16)
        qt = jnp.transpose(q[own, :].astype(f32))
        qn = qt * lax.rsqrt(jnp.sum(qt * qt, axis=0, keepdims=True) + 1e-6)
        xs[j] = jnp.zeros((E, HALF), f32)
        rs[j] = qn
        ds[j] = qn
        rr[j] = jnp.sum(qn * qn, axis=0, keepdims=True)

    def products(j, vector, weights, right):
        high, low = split(vector)
        y = dot(left[j], jnp.concatenate((high, low), axis=0))
        inside = two_part(right, weights * y[:HALF])
        return leads[j] * (y[HALF : HALF + E] + y[HALF + E :]) + inside

    def iteration(_, carry):
        for j in range(2):
            d = ds[j]
            image = products(j, d, mix[j], keys_t[j]) + RIDGE * d
            now = rr[j]
            alpha = now / jnp.maximum(jnp.sum(d * image, axis=0, keepdims=True), TINY)
            xs[j] = xs[j] + alpha * d
            r = rs[j] - alpha * image
            rs[j] = r
            new = jnp.sum(r * r, axis=0, keepdims=True)
            ds[j] = r + new / jnp.maximum(now, TINY) * d
            rr[j] = new
        return carry

    lax.fori_loop(0, CG_STEPS, iteration, 0)
    for j in range(2):
        own = slice(j * HALF, (j + 1) * HALF)
        high, low = split(starts[j][E:])
        left[j, HALF : HALF + E, :E] = high
        left[j, HALF : HALF + E, E:] = high
        left[j, HALF + E :, :E] = low
        vt = jnp.transpose(kv[1, own, :].astype(f32)).astype(bf16)
        out[:, own] = products(j, xs[j], mix_v[j], vt)


def attend_body(pos, q, kv, near, far, mesa, keep_out, c_out, z_out, cz_out, place):
    core, chip = pos[0], pos[1] * 4 + pos[2]
    scale = E ** (-0.5)
    row, col = iotas((HALF, HALF))
    parts = [(far, 0, 2), (far, 1, 2), (near, 0, 1), (near, 1, 1), (kv, 0, 0), (kv, 1, 0)]

    def rows_of(b, which):
        source, half, _ = parts[b]
        return source[which, half * HALF : (half + 1) * HALF, :]

    values_t = [jnp.transpose(rows_of(b, 1).astype(f32)).astype(bf16) for b in range(6)]
    for j in range(2):
        own = slice(j * HALF, (j + 1) * HALF)
        qj = q[own, :]
        scores = []
        for b in range(j, j + 5):
            s = lax.dot_general(
                rows_of(b, 0), qj, (((1,), (1,)), ((), ())), preferred_element_type=f32
            )
            if b == j:
                s = jnp.where(row > col, s, LOW)
            if b == j + 4:
                s = jnp.where(row <= col, s, LOW)
            if parts[b][2]:
                s = jnp.where(chip >= parts[b][2], s, LOW)
            scores.append(s)
        largest = scores[0]
        for s in scores[1:]:
            largest = jnp.maximum(largest, s)
        largest = jnp.max(largest, axis=0, keepdims=True)
        total = jnp.zeros((1, HALF), f32)
        result = jnp.zeros((E, HALF), f32)
        for b, s in zip(range(j, j + 5), scores):
            expo = jnp.exp((s - largest) * scale)
            total = total + jnp.sum(expo, axis=0, keepdims=True)
            result = result + dot(values_t[b], expo.astype(bf16))
        both = jnp.transpose(result / total + mesa[:, own]).astype(bf16)
        for slot in range(HALF // SLOT):
            at = slot // 2 * SLOT
            place[2 * j + slot % 2, at : at + SLOT, :] = both[slot * SLOT : (slot + 1) * SLOT]
    side = lax.rem(pos[3], 2)
    keep_out[...] = place[2 * core + side]
    c_out[...] = place[2 * (1 - core) + side]
    z_out[...] = place[2 * core + 1 - side]
    cz_out[...] = place[2 * (1 - core) + 1 - side]


def project_body(pos, keep, from_c, from_z, from_cz, own_weight, pair_weight, mine, s1, s2, s3, wide):
    core, mine_at = pos[0], lax.div(pos[3], 2)
    for piece, at in (
        (keep, core),
        (from_c, 1 - core),
        (from_z, 2 + core),
        (from_cz, 3 - core),
    ):
        wide[:, pl.ds(pl.multiple_of(at * E, E), E)] = piece[...]
    rows = jnp.concatenate(
        [
            wide[pl.ds(pl.multiple_of(lax.rem(mine_at + d, 4) * SLOT, SLOT), SLOT), :]
            for d in range(4)
        ],
        axis=0,
    )
    y = dot(rows[:, : 2 * E], own_weight[...]) + dot(rows[:, 2 * E :], pair_weight[...])
    mine[...] = y[:SLOT]
    for d, out in ((1, s1), (2, s2), (3, s3)):
        out[...] = y[d * SLOT : (d + 1) * SLOT].astype(bf16)


def swapped(x):
    return lax.ppermute(x, "c", [(0, 1), (1, 0)])


def turned(x, axis, by):
    return lax.ppermute(x, axis, [(i, (i + by) % 4) for i in range(4)])


def across(x, dc, dz):
    pairs = [(c * 8 + z, (c ^ dc) * 8 + (z ^ dz)) for c in range(2) for z in range(8)]
    return lax.ppermute(x, ("c", "z"), pairs)


def on_device(queries, keys, values, log_forget, strength, out_weight):
    core, x, y = (lax.axis_index(a) for a in ("c", "x", "y"))
    pos = jnp.stack((core, x, y, lax.axis_index("z"))).astype(jnp.int32)
    rows = jnp.stack((queries, keys, values))
    gates = jnp.stack((log_forget, strength), axis=1)
    front = core == 0
    keep = jnp.where(front, rows[:, :, 0], rows[:, :, 1])
    send = jnp.where(front, rows[:, :, 1], rows[:, :, 0])
    gate_keep = jnp.where(front, gates[0], gates[1])
    gate_send = jnp.where(front, gates[1], gates[0])
    q, kv, gates, local, first = call(
        gram_body,
        [
            ((CHIP, E), bf16),
            ((2, CHIP, E), bf16),
            ((8, HALF), f32),
            ((ROWS, E), bf16),
            ((2 * E, E), f32),
        ],
        [],
        1 << 26,
        pos,
        keep,
        swapped(send),
        gate_keep,
        swapped(gate_send),
    )
    around_y = [turned(local, "y", by) for by in (1, 2, 3)]
    pair_weight = across(out_weight, 0, 1)
    row_total, state, lead = call(
        row_body,
        [((ROWS, E), bf16), ((2 * E, E), f32), ((8, E), f32)],
        [((4, ROWS, E), bf16)],
        1 << 20,
        pos,
        local,
        *around_y,
    )
    around_x = [turned(row_total, "x", by) for by in (1, 2, 3)]
    halo, _ = lax.optimization_barrier((kv, row_total))
    halos = []
    for by in (1, 2):
        halos.append(
            lax.ppermute(halo, XY, [(i, i + by) for i in range(16) if i + by < 16])
        )
    (mesa,) = call(
        solve_body,
        [((E, CHIP), f32)],
        [
            ((2, CHIP, CHIP // 2), bf16),
            ((2, E, HALF), bf16),
            ((2, HALF, HALF), f32),
            ((2, HALF, HALF), f32),
            ((2, E, HALF), f32),
            ((2, E, HALF), f32),
            ((2, E, HALF), f32),
            ((2, 1, HALF), f32),
        ],
        1 << 30,
        pos,
        q,
        kv,
        gates,
        first,
        state,
        lead,
        *around_x,
    )
    kept, to_c, to_z, to_cz = call(
        attend_body,
        [((HALF // 2, E), bf16)] * 4,
        [((4, HALF // 2, E), bf16)],
        1 << 29,
        pos,
        q,
        kv,
        *halos,
        mesa,
    )
    mine, *sent = call(
        project_body,
        [((SLOT, 2048), f32)] + [((SLOT, 2048), bf16)] * 3,
        [((HALF // 2, 4 * E), bf16)],
        1 << 28,
        pos,
        kept,
        across(to_c, 1, 0),
        across(to_z, 0, 1),
        across(to_cz, 1, 1),
        out_weight,
        pair_weight,
    )
    total = mine
    for by, share in zip((2, 4, 6), sent):
        got = lax.ppermute(share, "z", [(i, (i + by) % 8) for i in range(8)])
        total = total + got.astype(f32)
    return total.astype(bf16)


def solution(mesh):
    grid = Mesh(mesh.devices.reshape(4, 4, 2, mesh.shape["head"]), ("x", "y", "c", "z"))
    in_specs = (
        P(SEQ, "z", None),
        P(SEQ, "z", None),
        P(SEQ, "z", None),
        P("z", SEQ),
        P("z", SEQ),
        P("z", None),
    )

    return jax.shard_map(
        on_device, mesh=grid, in_specs=in_specs, out_specs=P((*SEQ, "z"), None), check_vma=False
    )
```

```python
import jax
import jax.numpy as jnp
from jax import lax
from jax.experimental import pallas as pl
from jax.experimental.pallas import tpu as pltpu
from jax.sharding import Mesh
from jax.sharding import PartitionSpec as P

CG_STEPS = 6
RIDGE = 0.25
TINY = 1e-30
LOW = -1e30
HALF = 256
E = 128
CHIP = 2 * HALF
ROWS = 2 * E + 16
SLOT = 32
SLOTS = 8
GRANT = 16 << 20
SEQ = ("x", "y", "c")
XY = ("x", "y")
f32 = jnp.float32
bf16 = jnp.bfloat16


def spec(kind=pltpu.VMEM):
    return pl.BlockSpec(memory_space=kind)


def call(body, outs, scratch, flops, *args):
    return pl.pallas_call(
        body,
        out_shape=[jax.ShapeDtypeStruct(shape, kind) for shape, kind in outs],
        in_specs=[spec(pltpu.SMEM)] + [spec()] * (len(args) - 1),
        out_specs=[spec()] * len(outs),
        scratch_shapes=[pltpu.VMEM(shape, kind) for shape, kind in scratch],
        compiler_params=pltpu.CompilerParams(vmem_limit_bytes=GRANT),
        cost_estimate=pl.CostEstimate(flops=flops, bytes_accessed=1 << 20, transcendentals=0),
    )(*args)


def split(x):
    high = x.astype(bf16)
    return high, (x - high.astype(f32)).astype(bf16)


def dot(a, b):
    return jnp.dot(a, b, preferred_element_type=f32)


def two_part(a, b):
    high, low = split(b)
    return dot(a, high) + dot(a, low)


def iotas(shape):
    return lax.broadcasted_iota(jnp.int32, shape, 0), lax.broadcasted_iota(jnp.int32, shape, 1)


def payload(state, total):
    high, low = split(total)
    row, _ = iotas((16, E))
    tail = jnp.where(row == 0, high.astype(f32), jnp.where(row == 1, low.astype(f32), 0.0))
    return jnp.concatenate((state, tail), axis=0).astype(bf16)


def decay_row(tail):
    wide = tail.astype(f32)
    return wide[0:1, :] + wide[1:2, :]


def gram_body(pos, keep, recv, gate_keep, gate_recv, q_out, kv_out, gates_out, pay_out, first_out):
    core = pos[0]
    for source, which in ((keep, core), (recv, 1 - core)):
        rows = pl.ds(pl.multiple_of(which * HALF, HALF), HALF)
        q_out[rows, :] = source[0]
        kv_out[0, rows, :] = source[1]
        kv_out[1, rows, :] = source[2]
    a, b = gate_keep[...], gate_recv[...]
    first, second = jnp.where(core == 0, a, b), jnp.where(core == 0, b, a)
    forget = jnp.concatenate((first[0:1], second[0:1], jnp.zeros((6, HALF), f32)), axis=0)
    row, col = iotas((HALF, HALF))
    upto = (row <= col).astype(f32)
    sums = jnp.dot(forget, upto, preferred_element_type=f32, precision=lax.Precision.HIGHEST)
    gates_out[...] = jnp.concatenate(
        (sums[0:2], first[1:2], second[1:2], jnp.zeros((4, HALF), f32)), axis=0
    )
    grams = []
    for j in range(2):
        own = slice(j * HALF, (j + 1) * HALF)
        k = kv_out[0, own, :]
        kt = jnp.transpose(k.astype(f32))
        vt = jnp.transpose(kv_out[1, own, :].astype(f32))
        r = lax.rsqrt(jnp.sum(kt * kt, axis=0, keepdims=True) + 1e-6)
        weight = jnp.exp(sums[j : j + 1, HALF - 1 :] - sums[j : j + 1]) * gates_out[2 + j : 3 + j]
        left = jnp.concatenate((kt * (weight * r * r), vt * (weight * r)), axis=0)
        high, low = split(left)
        grams.append(dot(high, k) + dot(low, k))
    first_out[...] = grams[0]
    later = sums[1:2, HALF - 1 :]
    local = jnp.exp(later) * grams[0] + grams[1]
    pay_out[...] = payload(local, jnp.broadcast_to(sums[0:1, HALF - 1 :] + later, (1, E)))


def row_body(pos, own, r1, r2, r3, pay_out, state_out, lead_out, place):
    mine = pos[2]
    place[mine] = own[...]
    for distance, received in ((1, r1), (2, r2), (3, r3)):
        place[lax.rem(mine + 4 - distance, 4)] = received[...]
    decays = [decay_row(place[m, 2 * E :, :]) for m in range(4)]
    zero = jnp.zeros((1, E), f32)
    total = before = jnp.zeros((2 * E, E), f32)
    lead = zero
    for m in range(4):
        block = place[m, : 2 * E, :].astype(f32)
        step = jnp.exp(decays[m])
        total = step * total + block
        earlier = m < mine
        before = jnp.where(earlier, step * before + block, before)
        lead = jnp.where(earlier, lead + decays[m], lead)
    pay_out[...] = payload(total, decays[0] + decays[1] + decays[2] + decays[3])
    state_out[...] = before
    lead_out[...] = jnp.broadcast_to(lead, (8, E))


def solve_body(
    pos, q, kv, gates, first, state, lead, t1, t2, t3, out, left, keys_t, mix, mix_v, xs, rs, ds, rr
):
    line = pos[1]
    start = jnp.zeros((2 * E, E), f32)
    passed = jnp.zeros((1, E), f32)
    for distance, received in ((1, t1), (2, t2), (3, t3)):
        block = received[: 2 * E, :].astype(f32)
        start = jnp.where(line >= distance, start + jnp.exp(passed) * block, start)
        passed = passed + decay_row(received[2 * E :, :])
    start = jnp.exp(lead[0:1, :]) * start + state[...]
    starts = [start, jnp.exp(gates[0:1, HALF - 1 :]) * start + first[...]]
    row, col = iotas((HALF, HALF))
    causal = row <= col
    leads = []
    for j in range(2):
        own = slice(j * HALF, (j + 1) * HALF)
        k = kv[0, own, :]
        kt = jnp.transpose(k.astype(f32))
        keys_t[j] = kt.astype(bf16)
        r = lax.rsqrt(jnp.sum(kt * kt, axis=0, keepdims=True) + 1e-6)
        c = gates[j : j + 1, :]
        strength = gates[2 + j : 3 + j, :]
        line_of, _ = iotas((E, HALF))
        columns = jnp.transpose(
            jnp.where(
                line_of == 0, c, jnp.where(line_of == 1, strength * r * r, strength * r)
            )
        )
        gap = jnp.where(causal, c - columns[:, 0:1], 0.0)
        decay = jnp.where(causal, jnp.exp(gap), 0.0)
        mix[j] = decay * columns[:, 1:2]
        mix_v[j] = decay * columns[:, 2:3]
        leads.append(jnp.exp(c))
        left[j, :HALF, :E] = k
        left[j, :HALF, E:] = k
        high, low = split(starts[j][:E])
        left[j, HALF : HALF + E, :E] = high
        left[j, HALF : HALF + E, E:] = high
        left[j, HALF + E :, :E] = low
        left[j, HALF + E :, E:] = jnp.zeros((E, E), bf16)
        qt = jnp.transpose(q[own, :].astype(f32))
        qn = qt * lax.rsqrt(jnp.sum(qt * qt, axis=0, keepdims=True) + 1e-6)
        xs[j] = jnp.zeros((E, HALF), f32)
        rs[j] = qn
        ds[j] = qn
        rr[j] = jnp.sum(qn * qn, axis=0, keepdims=True)

    def products(j, vector, weights, right):
        high, low = split(vector)
        y = dot(left[j], jnp.concatenate((high, low), axis=0))
        inside = two_part(right, weights * y[:HALF])
        return leads[j] * (y[HALF : HALF + E] + y[HALF + E :]) + inside

    def iteration(_, carry):
        for j in range(2):
            d = ds[j]
            image = products(j, d, mix[j], keys_t[j]) + RIDGE * d
            now = rr[j]
            alpha = now / jnp.maximum(jnp.sum(d * image, axis=0, keepdims=True), TINY)
            xs[j] = xs[j] + alpha * d
            r = rs[j] - alpha * image
            rs[j] = r
            new = jnp.sum(r * r, axis=0, keepdims=True)
            ds[j] = r + new / jnp.maximum(now, TINY) * d
            rr[j] = new
        return carry

    lax.fori_loop(0, CG_STEPS, iteration, 0)
    for j in range(2):
        own = slice(j * HALF, (j + 1) * HALF)
        high, low = split(starts[j][E:])
        left[j, HALF : HALF + E, :E] = high
        left[j, HALF : HALF + E, E:] = high
        left[j, HALF + E :, :E] = low
        vt = jnp.transpose(kv[1, own, :].astype(f32)).astype(bf16)
        out[:, own] = products(j, xs[j], mix_v[j], vt)


def attend_body(pos, q, kv, near, far, mesa, keep_out, c_out, z_out, cz_out, place):
    core, chip = pos[0], pos[1] * 4 + pos[2]
    scale = E ** (-0.5)
    row, col = iotas((HALF, HALF))
    parts = [(far, 0, 2), (far, 1, 2), (near, 0, 1), (near, 1, 1), (kv, 0, 0), (kv, 1, 0)]

    def rows_of(b, which):
        source, half, _ = parts[b]
        return source[which, half * HALF : (half + 1) * HALF, :]

    values_t = [jnp.transpose(rows_of(b, 1).astype(f32)).astype(bf16) for b in range(6)]
    for j in range(2):
        own = slice(j * HALF, (j + 1) * HALF)
        qj = q[own, :]
        scores = []
        for b in range(j, j + 5):
            s = lax.dot_general(
                rows_of(b, 0), qj, (((1,), (1,)), ((), ())), preferred_element_type=f32
            )
            if b == j:
                s = jnp.where(row > col, s, LOW)
            if b == j + 4:
                s = jnp.where(row <= col, s, LOW)
            if parts[b][2]:
                s = jnp.where(chip >= parts[b][2], s, LOW)
            scores.append(s)
        largest = scores[0]
        for s in scores[1:]:
            largest = jnp.maximum(largest, s)
        largest = jnp.max(largest, axis=0, keepdims=True)
        total = jnp.zeros((1, HALF), f32)
        result = jnp.zeros((E, HALF), f32)
        for b, s in zip(range(j, j + 5), scores):
            expo = jnp.exp((s - largest) * scale)
            total = total + jnp.sum(expo, axis=0, keepdims=True)
            result = result + dot(values_t[b], expo.astype(bf16))
        both = jnp.transpose(result / total + mesa[:, own]).astype(bf16)
        for slot in range(SLOTS):
            place[SLOTS * j + slot] = both[slot * SLOT : (slot + 1) * SLOT]

    def piece(which, device):
        way = 2 * lax.rem(device, 2) - 1
        return jnp.concatenate(
            [
                place[SLOTS * which + lax.rem(device + way * away + SLOTS, SLOTS)]
                for away in range(SLOTS // 2)
            ],
            axis=0,
        )

    here = pos[3]
    there = here + 1 - 2 * lax.rem(here, 2)
    keep_out[...] = piece(core, here)
    c_out[...] = piece(1 - core, here)
    z_out[...] = piece(core, there)
    cz_out[...] = piece(1 - core, there)


def project_body(pos, keep, from_c, from_z, from_cz, own_weight, pair_weight, mine, s1, s2, s3, wide):
    core = pos[0]
    for piece, at in (
        (keep, core),
        (from_c, 1 - core),
        (from_z, 2 + core),
        (from_cz, 3 - core),
    ):
        wide[:, pl.ds(pl.multiple_of(at * E, E), E)] = piece[...]
    y = dot(wide[:, : 2 * E], own_weight[...]) + dot(wide[:, 2 * E :], pair_weight[...])
    mine[...] = y[:SLOT]
    for d, out in ((1, s1), (2, s2), (3, s3)):
        out[...] = y[d * SLOT : (d + 1) * SLOT].astype(bf16)


def beyond(x, by):
    return lax.ppermute(x, XY, [(i, (i + by) % 16) for i in range(16)])


def turned(x, axis, by):
    return lax.ppermute(x, axis, [(i, (i + by) % 4) for i in range(4)])


def across(x, dc, dz):
    pairs = [(c * 8 + z, (c ^ dc) * 8 + (z ^ dz)) for c in range(2) for z in range(8)]
    return lax.ppermute(x, ("c", "z"), pairs)


def on_device(queries, keys, values, log_forget, strength, out_weight):
    pos = jnp.stack([lax.axis_index(a) for a in ("c", "x", "y", "z")]).astype(jnp.int32)
    front = lax.axis_index("c") == 0
    rows = jnp.stack((queries, keys, values))
    gates = jnp.stack((log_forget, strength), axis=1)
    keep = jnp.where(front, rows[:, :, 0], rows[:, :, 1])
    send = jnp.where(front, rows[:, :, 1], rows[:, :, 0])
    gate_keep = jnp.where(front, gates[0], gates[1])
    gate_send = jnp.where(front, gates[1], gates[0])
    received = across(send, 1, 0)
    gate_received = across(gate_send, 1, 0)
    pair_weight = across(out_weight, 0, 1)
    q, kv, gates, local, first = call(
        gram_body,
        [
            ((CHIP, E), bf16),
            ((2, CHIP, E), bf16),
            ((8, HALF), f32),
            ((ROWS, E), bf16),
            ((2 * E, E), f32),
        ],
        [],
        1 << 26,
        pos,
        keep,
        received,
        gate_keep,
        gate_received,
    )
    around_y = [turned(local, "y", by) for by in (1, 2, 3)]
    halos = [beyond(kv, 1), beyond(kv, 2)]
    row_total, state, lead = call(
        row_body,
        [((ROWS, E), bf16), ((2 * E, E), f32), ((8, E), f32)],
        [((4, ROWS, E), bf16)],
        1 << 20,
        pos,
        local,
        *around_y,
    )
    around_x = [turned(row_total, "x", by) for by in (1, 2, 3)]
    (mesa,) = call(
        solve_body,
        [((E, CHIP), f32)],
        [
            ((2, CHIP, CHIP // 2), bf16),
            ((2, E, HALF), bf16),
            ((2, HALF, HALF), f32),
            ((2, HALF, HALF), f32),
            ((2, E, HALF), f32),
            ((2, E, HALF), f32),
            ((2, E, HALF), f32),
            ((2, 1, HALF), f32),
        ],
        1 << 30,
        pos,
        q,
        kv,
        gates,
        first,
        state,
        lead,
        *around_x,
    )
    kept, to_c, to_z, to_cz = call(
        attend_body,
        [((HALF // 2, E), bf16)] * 4,
        [((2 * SLOTS, SLOT, E), bf16)],
        1 << 29,
        pos,
        q,
        kv,
        *halos,
        mesa,
    )
    from_cz = across(to_cz, 1, 1)
    from_z = across(to_z, 0, 1)
    from_c = across(to_c, 1, 0)
    mine, *sent = call(
        project_body,
        [((SLOT, 2048), f32)] + [((SLOT, 2048), bf16)] * 3,
        [((HALF // 2, 4 * E), bf16)],
        1 << 28,
        pos,
        kept,
        from_c,
        from_z,
        from_cz,
        out_weight,
        pair_weight,
    )
    total = mine
    for away, share in reversed(list(enumerate(sent, 1))):
        pairs = [(z, (z + (2 * (z % 2) - 1) * away) % SLOTS) for z in range(SLOTS)]
        total = total + lax.ppermute(share, "z", pairs).astype(f32)
    return total.astype(bf16)


def solution(mesh):
    grid = Mesh(mesh.devices.reshape(4, 4, 2, mesh.shape["head"]), ("x", "y", "c", "z"))
    in_specs = (
        P(SEQ, "z", None),
        P(SEQ, "z", None),
        P(SEQ, "z", None),
        P("z", SEQ),
        P("z", SEQ),
        P("z", None),
    )

    return jax.shard_map(
        on_device, mesh=grid, in_specs=in_specs, out_specs=P((*SEQ, "z"), None), check_vma=False
    )
```

```python
import jax
import jax.numpy as jnp
from jax import lax
from jax.experimental import pallas as pl
from jax.experimental.pallas import tpu as pltpu
from jax.sharding import Mesh
from jax.sharding import PartitionSpec as P

CG_STEPS = 6
RIDGE = 0.25
TINY = 1e-30
LOW = -1e30
HALF = 256
E = 128
CHIP = 2 * HALF
ROWS = 2 * E + 16
SLOT = 32
SLOTS = 8
GRANT = 16 << 20
SEQ = ("x", "y", "c")
XY = ("x", "y")
f32 = jnp.float32
bf16 = jnp.bfloat16


def spec(kind=pltpu.VMEM):
    return pl.BlockSpec(memory_space=kind)


def call(body, outs, scratch, flops, *args):
    return pl.pallas_call(
        body,
        out_shape=[jax.ShapeDtypeStruct(shape, kind) for shape, kind in outs],
        in_specs=[spec()] * len(args),
        out_specs=[spec()] * len(outs),
        scratch_shapes=[pltpu.VMEM(shape, kind) for shape, kind in scratch],
        compiler_params=pltpu.CompilerParams(vmem_limit_bytes=GRANT),
        cost_estimate=pl.CostEstimate(flops=flops, bytes_accessed=1 << 20, transcendentals=0),
    )(*args)


def split(x):
    high = x.astype(bf16)
    return high, (x - high.astype(f32)).astype(bf16)


def dot(a, b):
    return jnp.dot(a, b, preferred_element_type=f32)


def two_part(a, b):
    high, low = split(b)
    return dot(a, high) + dot(a, low)


def iotas(shape):
    return lax.broadcasted_iota(jnp.int32, shape, 0), lax.broadcasted_iota(jnp.int32, shape, 1)


def payload(state, total):
    high, low = split(total)
    row, _ = iotas((16, E))
    tail = jnp.where(row == 0, high.astype(f32), jnp.where(row == 1, low.astype(f32), 0.0))
    return jnp.concatenate((state, tail), axis=0).astype(bf16)


def decay_row(tail):
    wide = tail.astype(f32)
    return wide[0:1, :] + wide[1:2, :]


def gram_body(keep, recv, gate_keep, gate_recv, q_out, kv_out, gates_out, pay_out, first_out):
    core = lax.axis_index("c")
    for source, which in ((keep, core), (recv, 1 - core)):
        rows = pl.ds(pl.multiple_of(which * HALF, HALF), HALF)
        q_out[rows, :] = source[0]
        kv_out[0, rows, :] = source[1]
        kv_out[1, rows, :] = source[2]
    a, b = gate_keep[...], gate_recv[...]
    first, second = jnp.where(core == 0, a, b), jnp.where(core == 0, b, a)
    forget = jnp.concatenate((first[0:1], second[0:1], jnp.zeros((6, HALF), f32)), axis=0)
    row, col = iotas((HALF, HALF))
    upto = (row <= col).astype(f32)
    sums = jnp.dot(forget, upto, preferred_element_type=f32, precision=lax.Precision.HIGHEST)
    gates_out[...] = jnp.concatenate(
        (sums[0:2], first[1:2], second[1:2], jnp.zeros((4, HALF), f32)), axis=0
    )
    grams = []
    for j in range(2):
        own = slice(j * HALF, (j + 1) * HALF)
        k = kv_out[0, own, :]
        kt = jnp.transpose(k.astype(f32))
        vt = jnp.transpose(kv_out[1, own, :].astype(f32))
        r = lax.rsqrt(jnp.sum(kt * kt, axis=0, keepdims=True) + 1e-6)
        weight = jnp.exp(sums[j : j + 1, HALF - 1 :] - sums[j : j + 1]) * gates_out[2 + j : 3 + j]
        left = jnp.concatenate((kt * (weight * r * r), vt * (weight * r)), axis=0)
        high, low = split(left)
        grams.append(dot(high, k) + dot(low, k))
    first_out[...] = grams[0]
    later = sums[1:2, HALF - 1 :]
    local = jnp.exp(later) * grams[0] + grams[1]
    pay_out[...] = payload(local, jnp.broadcast_to(sums[0:1, HALF - 1 :] + later, (1, E)))


def row_body(own, r1, r2, r3, pay_out, state_out, lead_out, place):
    mine = lax.axis_index("y")
    place[mine] = own[...]
    for distance, received in ((1, r1), (2, r2), (3, r3)):
        place[lax.rem(mine + 4 - distance, 4)] = received[...]
    decays = [decay_row(place[m, 2 * E :, :]) for m in range(4)]
    zero = jnp.zeros((1, E), f32)
    total = before = jnp.zeros((2 * E, E), f32)
    lead = zero
    for m in range(4):
        block = place[m, : 2 * E, :].astype(f32)
        step = jnp.exp(decays[m])
        total = step * total + block
        earlier = m < mine
        before = jnp.where(earlier, step * before + block, before)
        lead = jnp.where(earlier, lead + decays[m], lead)
    pay_out[...] = payload(total, decays[0] + decays[1] + decays[2] + decays[3])
    state_out[...] = before
    lead_out[...] = jnp.broadcast_to(lead, (8, E))


def prepare_body(q, kv, gates, mix, mix_v, keys_t, values_t, queries_t, leads):
    row, col = iotas((HALF, HALF))
    causal = row <= col
    line_of, _ = iotas((E, HALF))
    for j in range(2):
        own = slice(j * HALF, (j + 1) * HALF)
        kt = jnp.transpose(kv[0, own, :].astype(f32))
        keys_t[j] = kt.astype(bf16)
        values_t[j] = jnp.transpose(kv[1, own, :].astype(f32)).astype(bf16)
        r = lax.rsqrt(jnp.sum(kt * kt, axis=0, keepdims=True) + 1e-6)
        c = gates[j : j + 1, :]
        strength = gates[2 + j : 3 + j, :]
        columns = jnp.transpose(
            jnp.where(
                line_of == 0, c, jnp.where(line_of == 1, strength * r * r, strength * r)
            )
        )
        gap = jnp.where(causal, c - columns[:, 0:1], 0.0)
        decay = jnp.where(causal, jnp.exp(gap), 0.0)
        mix[j] = decay * columns[:, 1:2]
        mix_v[j] = decay * columns[:, 2:3]
        qt = jnp.transpose(q[own, :].astype(f32))
        queries_t[j] = qt * lax.rsqrt(jnp.sum(qt * qt, axis=0, keepdims=True) + 1e-6)
    leads[...] = jnp.exp(gates[...])


def place_state(left, j, state):
    high, low = split(state)
    left[j, HALF : HALF + E, :E] = high
    left[j, HALF : HALF + E, E:] = high
    left[j, HALF + E :, :E] = low
    left[j, HALF + E :, E:] = jnp.zeros((E, E), bf16)


def solve_body(
    kv, gates, first, state, lead, mix, mix_v, keys_t, values_t, queries_t, leads, t1, t2, t3,
    out, left, xs, rs, ds, rr,
):
    line = lax.axis_index("x")
    start = jnp.zeros((2 * E, E), f32)
    passed = jnp.zeros((1, E), f32)
    for distance, received in ((1, t1), (2, t2), (3, t3)):
        block = received[: 2 * E, :].astype(f32)
        start = jnp.where(line >= distance, start + jnp.exp(passed) * block, start)
        passed = passed + decay_row(received[2 * E :, :])
    start = jnp.exp(lead[0:1, :]) * start + state[...]
    starts = [start, jnp.exp(gates[0:1, HALF - 1 :]) * start + first[...]]
    for j in range(2):
        k = kv[0, j * HALF : (j + 1) * HALF, :]
        left[j, :HALF, :E] = k
        left[j, :HALF, E:] = k
        place_state(left, j, starts[j][:E])
        qn = queries_t[j]
        xs[j] = jnp.zeros((E, HALF), f32)
        rs[j] = qn
        ds[j] = qn
        rr[j] = jnp.sum(qn * qn, axis=0, keepdims=True)

    def products(j, vector, weights, right):
        high, low = split(vector)
        y = dot(left[j], jnp.concatenate((high, low), axis=0))
        inside = two_part(right, weights * y[:HALF])
        return leads[j : j + 1, :] * (y[HALF : HALF + E] + y[HALF + E :]) + inside

    def iteration(_, carry):
        for j in range(2):
            d = ds[j]
            image = products(j, d, mix[j], keys_t[j]) + RIDGE * d
            now = rr[j]
            alpha = now / jnp.maximum(jnp.sum(d * image, axis=0, keepdims=True), TINY)
            xs[j] = xs[j] + alpha * d
            r = rs[j] - alpha * image
            rs[j] = r
            new = jnp.sum(r * r, axis=0, keepdims=True)
            ds[j] = r + new / jnp.maximum(now, TINY) * d
            rr[j] = new
        return carry

    lax.fori_loop(0, CG_STEPS, iteration, 0)
    for j in range(2):
        place_state(left, j, starts[j][E:])
        out[:, j * HALF : (j + 1) * HALF] = products(j, xs[j], mix_v[j], values_t[j])


def attend_body(q, kv, near, far, mesa, keep_out, c_out, z_out, cz_out, place):
    core = lax.axis_index("c")
    chip = lax.axis_index("x") * 4 + lax.axis_index("y")
    scale = E ** (-0.5)
    row, col = iotas((HALF, HALF))
    parts = [(far, 0, 2), (far, 1, 2), (near, 0, 1), (near, 1, 1), (kv, 0, 0), (kv, 1, 0)]

    def rows_of(b, which):
        source, half, _ = parts[b]
        return source[which, half * HALF : (half + 1) * HALF, :]

    values_t = [jnp.transpose(rows_of(b, 1).astype(f32)).astype(bf16) for b in range(6)]
    for j in range(2):
        own = slice(j * HALF, (j + 1) * HALF)
        qj = q[own, :]
        scores = []
        for b in range(j, j + 5):
            s = lax.dot_general(
                rows_of(b, 0), qj, (((1,), (1,)), ((), ())), preferred_element_type=f32
            )
            if b == j:
                s = jnp.where(row > col, s, LOW)
            if b == j + 4:
                s = jnp.where(row <= col, s, LOW)
            if parts[b][2]:
                s = jnp.where(chip >= parts[b][2], s, LOW)
            scores.append(s)
        largest = scores[0]
        for s in scores[1:]:
            largest = jnp.maximum(largest, s)
        largest = jnp.max(largest, axis=0, keepdims=True)
        total = jnp.zeros((1, HALF), f32)
        result = jnp.zeros((E, HALF), f32)
        for b, s in zip(range(j, j + 5), scores):
            expo = jnp.exp((s - largest) * scale)
            total = total + jnp.sum(expo, axis=0, keepdims=True)
            result = result + dot(values_t[b], expo.astype(bf16))
        both = jnp.transpose(result / total + mesa[:, own]).astype(bf16)
        for slot in range(SLOTS):
            place[SLOTS * j + slot] = both[slot * SLOT : (slot + 1) * SLOT]

    def piece(which, device):
        way = 2 * lax.rem(device, 2) - 1
        return jnp.concatenate(
            [
                place[SLOTS * which + lax.rem(device + way * away + SLOTS, SLOTS)]
                for away in range(SLOTS // 2)
            ],
            axis=0,
        )

    here = lax.axis_index("z")
    there = here + 1 - 2 * lax.rem(here, 2)
    keep_out[...] = piece(core, here)
    c_out[...] = piece(1 - core, here)
    z_out[...] = piece(core, there)
    cz_out[...] = piece(1 - core, there)


def project_body(keep, from_c, from_z, from_cz, own_weight, pair_weight, mine, s1, s2, s3, wide):
    core = lax.axis_index("c")
    for piece, at in (
        (keep, core),
        (from_c, 1 - core),
        (from_z, 2 + core),
        (from_cz, 3 - core),
    ):
        wide[:, pl.ds(pl.multiple_of(at * E, E), E)] = piece[...]
    y = dot(wide[:, : 2 * E], own_weight[...]) + dot(wide[:, 2 * E :], pair_weight[...])
    mine[...] = y[:SLOT]
    for d, out in ((1, s1), (2, s2), (3, s3)):
        out[...] = y[d * SLOT : (d + 1) * SLOT].astype(bf16)


def beyond(x, by):
    return lax.ppermute(x, XY, [(i, (i + by) % 16) for i in range(16)])


def turned(x, axis, by):
    return lax.ppermute(x, axis, [(i, (i + by) % 4) for i in range(4)])


def across(x, dc, dz):
    pairs = [(c * 8 + z, (c ^ dc) * 8 + (z ^ dz)) for c in range(2) for z in range(8)]
    return lax.ppermute(x, ("c", "z"), pairs)


def on_device(queries, keys, values, log_forget, strength, out_weight):
    front = lax.axis_index("c") == 0
    rows = jnp.stack((queries, keys, values))
    gates = jnp.stack((log_forget, strength), axis=1)
    keep = jnp.where(front, rows[:, :, 0], rows[:, :, 1])
    send = jnp.where(front, rows[:, :, 1], rows[:, :, 0])
    gate_keep = jnp.where(front, gates[0], gates[1])
    gate_send = jnp.where(front, gates[1], gates[0])
    received = across(send, 1, 0)
    gate_received = across(gate_send, 1, 0)
    pair_weight = across(out_weight, 0, 1)
    q, kv, gates, local, first = call(
        gram_body,
        [
            ((CHIP, E), bf16),
            ((2, CHIP, E), bf16),
            ((8, HALF), f32),
            ((ROWS, E), bf16),
            ((2 * E, E), f32),
        ],
        [],
        1 << 26,
        keep,
        received,
        gate_keep,
        gate_received,
    )
    around_y = [turned(local, "y", by) for by in (1, 2, 3)]
    halos = [beyond(kv, 1), beyond(kv, 2)]
    row_total, state, lead = call(
        row_body,
        [((ROWS, E), bf16), ((2 * E, E), f32), ((8, E), f32)],
        [((4, ROWS, E), bf16)],
        1 << 20,
        local,
        *around_y,
    )
    around_x = [turned(row_total, "x", by) for by in (1, 2, 3)]
    prepared = call(
        prepare_body,
        [
            ((2, HALF, HALF), f32),
            ((2, HALF, HALF), f32),
            ((2, E, HALF), bf16),
            ((2, E, HALF), bf16),
            ((2, E, HALF), f32),
            ((8, HALF), f32),
        ],
        [],
        1 << 26,
        q,
        kv,
        gates,
    )
    (mesa,) = call(
        solve_body,
        [((E, CHIP), f32)],
        [
            ((2, CHIP, 2 * E), bf16),
            ((2, E, HALF), f32),
            ((2, E, HALF), f32),
            ((2, E, HALF), f32),
            ((2, 1, HALF), f32),
        ],
        1 << 30,
        kv,
        gates,
        first,
        state,
        lead,
        *prepared,
        *around_x,
    )
    kept, to_c, to_z, to_cz = call(
        attend_body,
        [((HALF // 2, E), bf16)] * 4,
        [((2 * SLOTS, SLOT, E), bf16)],
        1 << 29,
        q,
        kv,
        *halos,
        mesa,
    )
    from_cz = across(to_cz, 1, 1)
    from_z = across(to_z, 0, 1)
    from_c = across(to_c, 1, 0)
    mine, *sent = call(
        project_body,
        [((SLOT, 2048), f32)] + [((SLOT, 2048), bf16)] * 3,
        [((HALF // 2, 4 * E), bf16)],
        1 << 28,
        kept,
        from_c,
        from_z,
        from_cz,
        out_weight,
        pair_weight,
    )
    total = mine
    for away, share in reversed(list(enumerate(sent, 1))):
        pairs = [(z, (z + (2 * (z % 2) - 1) * away) % SLOTS) for z in range(SLOTS)]
        total = total + lax.ppermute(share, "z", pairs).astype(f32)
    return total.astype(bf16)


def solution(mesh):
    grid = Mesh(mesh.devices.reshape(4, 4, 2, mesh.shape["head"]), ("x", "y", "c", "z"))
    in_specs = (
        P(SEQ, "z", None),
        P(SEQ, "z", None),
        P(SEQ, "z", None),
        P("z", SEQ),
        P("z", SEQ),
        P("z", None),
    )

    return jax.shard_map(
        on_device, mesh=grid, in_specs=in_specs, out_specs=P((*SEQ, "z"), None), check_vma=False
    )
```

```python
import jax
import jax.numpy as jnp
from jax import lax
from jax.experimental import pallas as pl
from jax.experimental.pallas import tpu as pltpu
from jax.sharding import Mesh
from jax.sharding import PartitionSpec as P

CG_STEPS = 6
RIDGE = 0.25
TINY = 1e-30
LOW = -1e30
HALF = 256
E = 128
CHIP = 2 * HALF
ROWS = 2 * E + 16
SLOT = 32
SLOTS = 8
GRANT = 16 << 20
SEQ = ("x", "y", "c")
XY = ("x", "y")
f32 = jnp.float32
bf16 = jnp.bfloat16


def spec(kind=pltpu.VMEM):
    return pl.BlockSpec(memory_space=kind)


def call(body, outs, scratch, flops, *args):
    return pl.pallas_call(
        body,
        out_shape=[jax.ShapeDtypeStruct(shape, kind) for shape, kind in outs],
        in_specs=[spec()] * len(args),
        out_specs=[spec()] * len(outs),
        scratch_shapes=[pltpu.VMEM(shape, kind) for shape, kind in scratch],
        compiler_params=pltpu.CompilerParams(vmem_limit_bytes=GRANT),
        cost_estimate=pl.CostEstimate(flops=flops, bytes_accessed=1 << 20, transcendentals=0),
    )(*args)


def split(x):
    high = x.astype(bf16)
    return high, (x - high.astype(f32)).astype(bf16)


def dot(a, b):
    return jnp.dot(a, b, preferred_element_type=f32)


def two_part(a, b):
    high, low = split(b)
    return dot(a, high) + dot(a, low)


def iotas(shape):
    return lax.broadcasted_iota(jnp.int32, shape, 0), lax.broadcasted_iota(jnp.int32, shape, 1)


def payload(state, total):
    high, low = split(total)
    row, _ = iotas((16, E))
    tail = jnp.where(row == 0, high.astype(f32), jnp.where(row == 1, low.astype(f32), 0.0))
    return jnp.concatenate((state, tail), axis=0).astype(bf16)


def decay_row(tail):
    wide = tail.astype(f32)
    return wide[0:1, :] + wide[1:2, :]


def gram_body(keep, recv, gate_keep, gate_recv, q_out, kv_out, gates_out, pay_out, first_out):
    core = lax.axis_index("c")
    for source, which in ((keep, core), (recv, 1 - core)):
        rows = pl.ds(pl.multiple_of(which * HALF, HALF), HALF)
        q_out[rows, :] = source[0]
        kv_out[0, rows, :] = source[1]
        kv_out[1, rows, :] = source[2]
    a, b = gate_keep[...], gate_recv[...]
    first, second = jnp.where(core == 0, a, b), jnp.where(core == 0, b, a)
    forget = jnp.concatenate((first[0:1], second[0:1], jnp.zeros((6, HALF), f32)), axis=0)
    row, col = iotas((HALF, HALF))
    upto = (row <= col).astype(f32)
    sums = jnp.dot(forget, upto, preferred_element_type=f32, precision=lax.Precision.HIGHEST)
    gates_out[...] = jnp.concatenate(
        (sums[0:2], first[1:2], second[1:2], jnp.zeros((4, HALF), f32)), axis=0
    )
    grams = []
    for j in range(2):
        own = slice(j * HALF, (j + 1) * HALF)
        k = kv_out[0, own, :]
        kt = jnp.transpose(k.astype(f32))
        vt = jnp.transpose(kv_out[1, own, :].astype(f32))
        r = lax.rsqrt(jnp.sum(kt * kt, axis=0, keepdims=True) + 1e-6)
        weight = jnp.exp(sums[j : j + 1, HALF - 1 :] - sums[j : j + 1]) * gates_out[2 + j : 3 + j]
        left = jnp.concatenate((kt * (weight * r * r), vt * (weight * r)), axis=0)
        high, low = split(left)
        grams.append(dot(high, k) + dot(low, k))
    first_out[...] = grams[0]
    later = sums[1:2, HALF - 1 :]
    local = jnp.exp(later) * grams[0] + grams[1]
    pay_out[...] = payload(local, jnp.broadcast_to(sums[0:1, HALF - 1 :] + later, (1, E)))


def row_body(own, r1, r2, r3, pay_out, state_out, lead_out, place):
    mine = lax.axis_index("y")
    place[mine] = own[...]
    for distance, received in ((1, r1), (2, r2), (3, r3)):
        place[lax.rem(mine + 4 - distance, 4)] = received[...]
    decays = [decay_row(place[m, 2 * E :, :]) for m in range(4)]
    zero = jnp.zeros((1, E), f32)
    total = before = jnp.zeros((2 * E, E), f32)
    lead = zero
    for m in range(4):
        block = place[m, : 2 * E, :].astype(f32)
        step = jnp.exp(decays[m])
        total = step * total + block
        earlier = m < mine
        before = jnp.where(earlier, step * before + block, before)
        lead = jnp.where(earlier, lead + decays[m], lead)
    pay_out[...] = payload(total, decays[0] + decays[1] + decays[2] + decays[3])
    state_out[...] = before
    lead_out[...] = jnp.broadcast_to(lead, (8, E))


def prepare_body(q, kv, gates, mix, mix_v, keys_t, values_t, queries_t, leads):
    row, col = iotas((HALF, HALF))
    causal = row <= col
    line_of, _ = iotas((E, HALF))
    for j in range(2):
        own = slice(j * HALF, (j + 1) * HALF)
        kt = jnp.transpose(kv[0, own, :].astype(f32))
        keys_t[j] = kt.astype(bf16)
        values_t[j] = jnp.transpose(kv[1, own, :].astype(f32)).astype(bf16)
        r = lax.rsqrt(jnp.sum(kt * kt, axis=0, keepdims=True) + 1e-6)
        c = gates[j : j + 1, :]
        strength = gates[2 + j : 3 + j, :]
        columns = jnp.transpose(
            jnp.where(
                line_of == 0, c, jnp.where(line_of == 1, strength * r * r, strength * r)
            )
        )
        gap = jnp.where(causal, c - columns[:, 0:1], 0.0)
        decay = jnp.where(causal, jnp.exp(gap), 0.0)
        mix[j] = decay * columns[:, 1:2]
        mix_v[j] = decay * columns[:, 2:3]
        qt = jnp.transpose(q[own, :].astype(f32))
        queries_t[j] = qt * lax.rsqrt(jnp.sum(qt * qt, axis=0, keepdims=True) + 1e-6)
    leads[...] = jnp.exp(gates[...])


def place_state(left, j, state):
    high, low = split(state)
    left[j, HALF : HALF + E, :E] = high
    left[j, HALF : HALF + E, E:] = high
    left[j, HALF + E :, :E] = low
    left[j, HALF + E :, E:] = jnp.zeros((E, E), bf16)


def solve_body(
    kv, gates, first, state, lead, mix, mix_v, keys_t, values_t, queries_t, leads, t1, t2, t3,
    out, left,
):
    line = lax.axis_index("x")
    start = jnp.zeros((2 * E, E), f32)
    passed = jnp.zeros((1, E), f32)
    for distance, received in ((1, t1), (2, t2), (3, t3)):
        block = received[: 2 * E, :].astype(f32)
        start = jnp.where(line >= distance, start + jnp.exp(passed) * block, start)
        passed = passed + decay_row(received[2 * E :, :])
    start = jnp.exp(lead[0:1, :]) * start + state[...]
    starts = [start, jnp.exp(gates[0:1, HALF - 1 :]) * start + first[...]]
    for j in range(2):
        k = kv[0, j * HALF : (j + 1) * HALF, :]
        left[j, :HALF, :E] = k
        left[j, :HALF, E:] = k
        place_state(left, j, starts[j][:E])

    def products(j, vector, weights, right):
        high, low = split(vector)
        y = dot(left[j], jnp.concatenate((high, low), axis=0))
        inside = two_part(right, weights * y[:HALF])
        return leads[j : j + 1, :] * (y[HALF : HALF + E] + y[HALF + E :]) + inside

    xs = [jnp.zeros((E, HALF), f32)] * 2
    rs = [queries_t[j] for j in range(2)]
    ds = list(rs)
    norms = [jnp.sum(r * r, axis=0, keepdims=True) for r in rs]
    for _ in range(CG_STEPS):
        for j in range(2):
            d = ds[j]
            image = products(j, d, mix[j], keys_t[j]) + RIDGE * d
            alpha = norms[j] / jnp.maximum(jnp.sum(d * image, axis=0, keepdims=True), TINY)
            xs[j] = xs[j] + alpha * d
            rs[j] = rs[j] - alpha * image
            new = jnp.sum(rs[j] * rs[j], axis=0, keepdims=True)
            ds[j] = rs[j] + new / jnp.maximum(norms[j], TINY) * d
            norms[j] = new
    for j in range(2):
        place_state(left, j, starts[j][E:])
        out[:, j * HALF : (j + 1) * HALF] = products(j, xs[j], mix_v[j], values_t[j])


def attend_body(q, kv, near, far, mesa, keep_out, c_out, z_out, cz_out, place):
    core = lax.axis_index("c")
    chip = lax.axis_index("x") * 4 + lax.axis_index("y")
    scale = E ** (-0.5)
    row, col = iotas((HALF, HALF))
    parts = [(far, 0, 2), (far, 1, 2), (near, 0, 1), (near, 1, 1), (kv, 0, 0), (kv, 1, 0)]

    def rows_of(b, which):
        source, half, _ = parts[b]
        return source[which, half * HALF : (half + 1) * HALF, :]

    values_t = [jnp.transpose(rows_of(b, 1).astype(f32)).astype(bf16) for b in range(6)]
    for j in range(2):
        own = slice(j * HALF, (j + 1) * HALF)
        qj = q[own, :]
        scores = []
        for b in range(j, j + 5):
            s = lax.dot_general(
                rows_of(b, 0), qj, (((1,), (1,)), ((), ())), preferred_element_type=f32
            )
            if b == j:
                s = jnp.where(row > col, s, LOW)
            if b == j + 4:
                s = jnp.where(row <= col, s, LOW)
            if parts[b][2]:
                s = jnp.where(chip >= parts[b][2], s, LOW)
            scores.append(s)
        largest = scores[0]
        for s in scores[1:]:
            largest = jnp.maximum(largest, s)
        largest = jnp.max(largest, axis=0, keepdims=True)
        total = jnp.zeros((1, HALF), f32)
        result = jnp.zeros((E, HALF), f32)
        for b, s in zip(range(j, j + 5), scores):
            expo = jnp.exp((s - largest) * scale)
            total = total + jnp.sum(expo, axis=0, keepdims=True)
            result = result + dot(values_t[b], expo.astype(bf16))
        both = jnp.transpose(result / total + mesa[:, own]).astype(bf16)
        for slot in range(SLOTS):
            place[SLOTS * j + slot] = both[slot * SLOT : (slot + 1) * SLOT]

    def piece(which, device):
        way = 2 * lax.rem(device, 2) - 1
        return jnp.concatenate(
            [
                place[SLOTS * which + lax.rem(device + way * away + SLOTS, SLOTS)]
                for away in range(SLOTS // 2)
            ],
            axis=0,
        )

    here = lax.axis_index("z")
    there = here + 1 - 2 * lax.rem(here, 2)
    keep_out[...] = piece(core, here)
    c_out[...] = piece(1 - core, here)
    z_out[...] = piece(core, there)
    cz_out[...] = piece(1 - core, there)


def project_body(keep, from_c, from_z, from_cz, own_weight, pair_weight, mine, s1, s2, s3, wide):
    core = lax.axis_index("c")
    for piece, at in (
        (keep, core),
        (from_c, 1 - core),
        (from_z, 2 + core),
        (from_cz, 3 - core),
    ):
        wide[:, pl.ds(pl.multiple_of(at * E, E), E)] = piece[...]
    y = dot(wide[:, : 2 * E], own_weight[...]) + dot(wide[:, 2 * E :], pair_weight[...])
    mine[...] = y[:SLOT]
    for d, out in ((1, s1), (2, s2), (3, s3)):
        out[...] = y[d * SLOT : (d + 1) * SLOT].astype(bf16)


def sum_body(mine, a, b, c, out):
    out[...] = (mine[...] + a[...].astype(f32) + b[...].astype(f32) + c[...].astype(f32)).astype(
        bf16
    )


def beyond(x, by):
    return lax.ppermute(x, XY, [(i, (i + by) % 16) for i in range(16)])


def turned(x, axis, by):
    return lax.ppermute(x, axis, [(i, (i + by) % 4) for i in range(4)])


def across(x, dc, dz):
    pairs = [(c * 8 + z, (c ^ dc) * 8 + (z ^ dz)) for c in range(2) for z in range(8)]
    return lax.ppermute(x, ("c", "z"), pairs)


def on_device(queries, keys, values, log_forget, strength, out_weight):
    front = lax.axis_index("c") == 0
    rows = jnp.stack((queries, keys, values))
    gates = jnp.stack((log_forget, strength), axis=1)
    keep = jnp.where(front, rows[:, :, 0], rows[:, :, 1])
    send = jnp.where(front, rows[:, :, 1], rows[:, :, 0])
    gate_keep = jnp.where(front, gates[0], gates[1])
    gate_send = jnp.where(front, gates[1], gates[0])
    received = across(send, 1, 0)
    gate_received = across(gate_send, 1, 0)
    pair_weight = across(out_weight, 0, 1)
    q, kv, gates, local, first = call(
        gram_body,
        [
            ((CHIP, E), bf16),
            ((2, CHIP, E), bf16),
            ((8, HALF), f32),
            ((ROWS, E), bf16),
            ((2 * E, E), f32),
        ],
        [],
        1 << 26,
        keep,
        received,
        gate_keep,
        gate_received,
    )
    around_y = [turned(local, "y", by) for by in (1, 2, 3)]
    halos = [beyond(kv, 1), beyond(kv, 2)]
    row_total, state, lead = call(
        row_body,
        [((ROWS, E), bf16), ((2 * E, E), f32), ((8, E), f32)],
        [((4, ROWS, E), bf16)],
        1 << 20,
        local,
        *around_y,
    )
    around_x = [turned(row_total, "x", by) for by in (1, 2, 3)]
    prepared = call(
        prepare_body,
        [
            ((2, HALF, HALF), f32),
            ((2, HALF, HALF), f32),
            ((2, E, HALF), bf16),
            ((2, E, HALF), bf16),
            ((2, E, HALF), f32),
            ((8, HALF), f32),
        ],
        [],
        1 << 26,
        q,
        kv,
        gates,
    )
    (mesa,) = call(
        solve_body,
        [((E, CHIP), f32)],
        [
            ((2, CHIP, 2 * E), bf16),
        ],
        1 << 30,
        kv,
        gates,
        first,
        state,
        lead,
        *prepared,
        *around_x,
    )
    kept, to_c, to_z, to_cz = call(
        attend_body,
        [((HALF // 2, E), bf16)] * 4,
        [((2 * SLOTS, SLOT, E), bf16)],
        1 << 29,
        q,
        kv,
        *halos,
        mesa,
    )
    from_cz = across(to_cz, 1, 1)
    from_z = across(to_z, 0, 1)
    from_c = across(to_c, 1, 0)
    mine, *sent = call(
        project_body,
        [((SLOT, 2048), f32)] + [((SLOT, 2048), bf16)] * 3,
        [((HALF // 2, 4 * E), bf16)],
        1 << 28,
        kept,
        from_c,
        from_z,
        from_cz,
        out_weight,
        pair_weight,
    )
    got = []
    for away, share in reversed(list(enumerate(sent, 1))):
        pairs = [(z, (z + (2 * (z % 2) - 1) * away) % SLOTS) for z in range(SLOTS)]
        got.append(lax.ppermute(share, "z", pairs))
    (total,) = call(sum_body, [((SLOT, 2048), bf16)], [], 1 << 18, mine, *got)
    return total


def solution(mesh):
    grid = Mesh(mesh.devices.reshape(4, 4, 2, mesh.shape["head"]), ("x", "y", "c", "z"))
    in_specs = (
        P(SEQ, "z", None),
        P(SEQ, "z", None),
        P(SEQ, "z", None),
        P("z", SEQ),
        P("z", SEQ),
        P("z", None),
    )

    return jax.shard_map(
        on_device, mesh=grid, in_specs=in_specs, out_specs=P((*SEQ, "z"), None), check_vma=False
    )
```

```python
import jax
import jax.numpy as jnp
from jax import lax
from jax.experimental import pallas as pl
from jax.experimental.pallas import tpu as pltpu
from jax.sharding import Mesh
from jax.sharding import PartitionSpec as P

CG_STEPS = 6
RIDGE = 0.25
TINY = 1e-30
LOW = -1e30
HALF = 256
E = 128
CHIP = 2 * HALF
SIDE = E // 2
BODY = SIDE + E
ROWS = BODY + 16
SLOT = 32
SLOTS = 8
GRANT = 16 << 20
SEQ = ("x", "y", "c")
XY = ("x", "y")
f32 = jnp.float32
bf16 = jnp.bfloat16


def spec(kind=pltpu.VMEM):
    return pl.BlockSpec(memory_space=kind)


def call(body, outs, scratch, flops, *args):
    return pl.pallas_call(
        body,
        out_shape=[jax.ShapeDtypeStruct(shape, kind) for shape, kind in outs],
        in_specs=[spec()] * len(args),
        out_specs=[spec()] * len(outs),
        scratch_shapes=[pltpu.VMEM(shape, kind) for shape, kind in scratch],
        compiler_params=pltpu.CompilerParams(vmem_limit_bytes=GRANT),
        cost_estimate=pl.CostEstimate(flops=flops, bytes_accessed=1 << 20, transcendentals=0),
    )(*args)


def split(x):
    high = x.astype(bf16)
    return high, (x - high.astype(f32)).astype(bf16)


def dot(a, b):
    return jnp.dot(a, b, preferred_element_type=f32)


def two_part(a, b):
    high, low = split(b)
    return dot(a, high) + dot(a, low)


def iotas(shape):
    return lax.broadcasted_iota(jnp.int32, shape, 0), lax.broadcasted_iota(jnp.int32, shape, 1)


def packed(state):
    top, bottom = state[:SIDE], pltpu.roll(state[SIDE:E], SIDE, 1)
    row, col = iotas((SIDE, E))
    square = jnp.where((col < SIDE) & (row < col), bottom, top)
    diagonal = jnp.sum(jnp.where(row == col, bottom, 0.0), axis=0, keepdims=True)
    line, _ = iotas((16, E))
    return jnp.concatenate((square, state[E:], jnp.where(line == 2, diagonal, 0.0)), axis=0)


def unpacked(state):
    square, diagonal = state[:SIDE], state[BODY + 2 : BODY + 3]
    turned_square = jnp.transpose(jnp.concatenate((square, jnp.zeros((SIDE, E), f32)), axis=0))
    other = turned_square[:SIDE]
    row, col = iotas((SIDE, E))
    top = jnp.where((col < SIDE) & (row < col), other, square)
    corner = jnp.where(row < col, square, jnp.where(row > col, other, diagonal))
    bottom = jnp.where(col < SIDE, turned_square[SIDE:], pltpu.roll(corner, SIDE, 1))
    return jnp.concatenate((top, bottom, state[SIDE:BODY]), axis=0)


def payload(state, total):
    high, low = split(total)
    row, _ = iotas((16, E))
    tail = jnp.where(
        row == 0, high.astype(f32), jnp.where(row == 1, low.astype(f32), state[BODY:])
    )
    return jnp.concatenate((state[:BODY], tail), axis=0).astype(bf16)


def decay_row(tail):
    wide = tail.astype(f32)
    return wide[0:1, :] + wide[1:2, :]


def gram_body(keep, recv, gate_keep, gate_recv, q_out, kv_out, gates_out, pay_out, first_out):
    core = lax.axis_index("c")
    for source, which in ((keep, core), (recv, 1 - core)):
        rows = pl.ds(pl.multiple_of(which * HALF, HALF), HALF)
        q_out[rows, :] = source[0]
        kv_out[0, rows, :] = source[1]
        kv_out[1, rows, :] = source[2]
    a, b = gate_keep[...], gate_recv[...]
    first, second = jnp.where(core == 0, a, b), jnp.where(core == 0, b, a)
    forget = jnp.concatenate((first[0:1], second[0:1], jnp.zeros((6, HALF), f32)), axis=0)
    row, col = iotas((HALF, HALF))
    upto = (row <= col).astype(f32)
    sums = jnp.dot(forget, upto, preferred_element_type=f32, precision=lax.Precision.HIGHEST)
    gates_out[...] = jnp.concatenate(
        (sums[0:2], first[1:2], second[1:2], jnp.zeros((4, HALF), f32)), axis=0
    )
    grams = []
    for j in range(2):
        own = slice(j * HALF, (j + 1) * HALF)
        k = kv_out[0, own, :]
        kt = jnp.transpose(k.astype(f32))
        vt = jnp.transpose(kv_out[1, own, :].astype(f32))
        r = lax.rsqrt(jnp.sum(kt * kt, axis=0, keepdims=True) + 1e-6)
        weight = jnp.exp(sums[j : j + 1, HALF - 1 :] - sums[j : j + 1]) * gates_out[2 + j : 3 + j]
        left = jnp.concatenate((kt * (weight * r * r), vt * (weight * r)), axis=0)
        high, low = split(left)
        grams.append(dot(high, k) + dot(low, k))
    first_out[...] = grams[0]
    later = sums[1:2, HALF - 1 :]
    local = jnp.exp(later) * grams[0] + grams[1]
    pay_out[...] = payload(packed(local), jnp.broadcast_to(sums[0:1, HALF - 1 :] + later, (1, E)))


def row_body(own, r1, r2, r3, pay_out, state_out, lead_out, place):
    mine = lax.axis_index("y")
    place[mine] = own[...]
    for distance, received in ((1, r1), (2, r2), (3, r3)):
        place[lax.rem(mine + 4 - distance, 4)] = received[...]
    decays = [decay_row(place[m, BODY:, :]) for m in range(4)]
    zero = jnp.zeros((1, E), f32)
    total = before = jnp.zeros((ROWS, E), f32)
    lead = zero
    for m in range(4):
        block = place[m].astype(f32)
        step = jnp.exp(decays[m])
        total = step * total + block
        earlier = m < mine
        before = jnp.where(earlier, step * before + block, before)
        lead = jnp.where(earlier, lead + decays[m], lead)
    pay_out[...] = payload(total, decays[0] + decays[1] + decays[2] + decays[3])
    state_out[...] = before
    lead_out[...] = jnp.broadcast_to(lead, (8, E))


def prepare_body(q, kv, gates, mix, mix_v, keys_t, values_t, queries_t, leads):
    row, col = iotas((HALF, HALF))
    causal = row <= col
    line_of, _ = iotas((E, HALF))
    for j in range(2):
        own = slice(j * HALF, (j + 1) * HALF)
        kt = jnp.transpose(kv[0, own, :].astype(f32))
        keys_t[j] = kt.astype(bf16)
        values_t[j] = jnp.transpose(kv[1, own, :].astype(f32)).astype(bf16)
        r = lax.rsqrt(jnp.sum(kt * kt, axis=0, keepdims=True) + 1e-6)
        c = gates[j : j + 1, :]
        strength = gates[2 + j : 3 + j, :]
        columns = jnp.transpose(
            jnp.where(
                line_of == 0, c, jnp.where(line_of == 1, strength * r * r, strength * r)
            )
        )
        gap = jnp.where(causal, c - columns[:, 0:1], 0.0)
        decay = jnp.where(causal, jnp.exp(gap), 0.0)
        mix[j] = decay * columns[:, 1:2]
        mix_v[j] = decay * columns[:, 2:3]
        qt = jnp.transpose(q[own, :].astype(f32))
        queries_t[j] = qt * lax.rsqrt(jnp.sum(qt * qt, axis=0, keepdims=True) + 1e-6)
    leads[...] = jnp.exp(gates[...])


def place_state(left, j, state):
    high, low = split(state)
    left[j, HALF : HALF + E, :E] = high
    left[j, HALF : HALF + E, E:] = high
    left[j, HALF + E :, :E] = low
    left[j, HALF + E :, E:] = jnp.zeros((E, E), bf16)


def solve_body(
    kv, gates, first, state, lead, mix, mix_v, keys_t, values_t, queries_t, leads, t1, t2, t3,
    out, left,
):
    line = lax.axis_index("x")
    start = jnp.zeros((ROWS, E), f32)
    passed = jnp.zeros((1, E), f32)
    for distance, received in ((1, t1), (2, t2), (3, t3)):
        block = received[...].astype(f32)
        start = jnp.where(line >= distance, start + jnp.exp(passed) * block, start)
        passed = passed + decay_row(received[BODY:, :])
    start = unpacked(jnp.exp(lead[0:1, :]) * start + state[...])
    starts = [start, jnp.exp(gates[0:1, HALF - 1 :]) * start + first[...]]
    for j in range(2):
        k = kv[0, j * HALF : (j + 1) * HALF, :]
        left[j, :HALF, :E] = k
        left[j, :HALF, E:] = k
        place_state(left, j, starts[j][:E])

    def products(j, vector, weights, right):
        high, low = split(vector)
        y = dot(left[j], jnp.concatenate((high, low), axis=0))
        inside = two_part(right, weights * y[:HALF])
        return leads[j : j + 1, :] * (y[HALF : HALF + E] + y[HALF + E :]) + inside

    xs = [jnp.zeros((E, HALF), f32)] * 2
    rs = [queries_t[j] for j in range(2)]
    ds = list(rs)
    norms = [jnp.sum(r * r, axis=0, keepdims=True) for r in rs]
    for _ in range(CG_STEPS):
        for j in range(2):
            d = ds[j]
            image = products(j, d, mix[j], keys_t[j]) + RIDGE * d
            alpha = norms[j] / jnp.maximum(jnp.sum(d * image, axis=0, keepdims=True), TINY)
            xs[j] = xs[j] + alpha * d
            rs[j] = rs[j] - alpha * image
            new = jnp.sum(rs[j] * rs[j], axis=0, keepdims=True)
            ds[j] = rs[j] + new / jnp.maximum(norms[j], TINY) * d
            norms[j] = new
    for j in range(2):
        place_state(left, j, starts[j][E:])
        out[:, j * HALF : (j + 1) * HALF] = products(j, xs[j], mix_v[j], values_t[j])


def attend_body(q, kv, near, far, mesa, keep_out, c_out, z_out, cz_out, place):
    core = lax.axis_index("c")
    chip = lax.axis_index("x") * 4 + lax.axis_index("y")
    scale = E ** (-0.5)
    row, col = iotas((HALF, HALF))
    parts = [(far, 0, 2), (far, 1, 2), (near, 0, 1), (near, 1, 1), (kv, 0, 0), (kv, 1, 0)]

    def rows_of(b, which):
        source, half, _ = parts[b]
        return source[which, half * HALF : (half + 1) * HALF, :]

    values_t = [jnp.transpose(rows_of(b, 1).astype(f32)).astype(bf16) for b in range(6)]
    for j in range(2):
        own = slice(j * HALF, (j + 1) * HALF)
        qj = q[own, :]
        scores = []
        for b in range(j, j + 5):
            s = lax.dot_general(
                rows_of(b, 0), qj, (((1,), (1,)), ((), ())), preferred_element_type=f32
            )
            if b == j:
                s = jnp.where(row > col, s, LOW)
            if b == j + 4:
                s = jnp.where(row <= col, s, LOW)
            if parts[b][2]:
                s = jnp.where(chip >= parts[b][2], s, LOW)
            scores.append(s)
        largest = scores[0]
        for s in scores[1:]:
            largest = jnp.maximum(largest, s)
        largest = jnp.max(largest, axis=0, keepdims=True)
        total = jnp.zeros((1, HALF), f32)
        result = jnp.zeros((E, HALF), f32)
        for b, s in zip(range(j, j + 5), scores):
            expo = jnp.exp((s - largest) * scale)
            total = total + jnp.sum(expo, axis=0, keepdims=True)
            result = result + dot(values_t[b], expo.astype(bf16))
        both = jnp.transpose(result / total + mesa[:, own]).astype(bf16)
        for slot in range(SLOTS):
            place[SLOTS * j + slot] = both[slot * SLOT : (slot + 1) * SLOT]

    def piece(which, device):
        way = 2 * lax.rem(device, 2) - 1
        return jnp.concatenate(
            [
                place[SLOTS * which + lax.rem(device + way * away + SLOTS, SLOTS)]
                for away in range(SLOTS // 2)
            ],
            axis=0,
        )

    here = lax.axis_index("z")
    there = here + 1 - 2 * lax.rem(here, 2)
    keep_out[...] = piece(core, here)
    c_out[...] = piece(1 - core, here)
    z_out[...] = piece(core, there)
    cz_out[...] = piece(1 - core, there)


def project_body(keep, from_c, from_z, from_cz, own_weight, pair_weight, mine, s1, s2, s3, wide):
    core = lax.axis_index("c")
    for piece, at in (
        (keep, core),
        (from_c, 1 - core),
        (from_z, 2 + core),
        (from_cz, 3 - core),
    ):
        wide[:, pl.ds(pl.multiple_of(at * E, E), E)] = piece[...]
    y = dot(wide[:, : 2 * E], own_weight[...]) + dot(wide[:, 2 * E :], pair_weight[...])
    mine[...] = y[:SLOT]
    for d, out in ((1, s1), (2, s2), (3, s3)):
        out[...] = y[d * SLOT : (d + 1) * SLOT].astype(bf16)


def sum_body(mine, a, b, c, out):
    out[...] = (mine[...] + a[...].astype(f32) + b[...].astype(f32) + c[...].astype(f32)).astype(
        bf16
    )


def beyond(x, by):
    return lax.ppermute(x, XY, [(i, (i + by) % 16) for i in range(16)])


def turned(x, axis, by):
    return lax.ppermute(x, axis, [(i, (i + by) % 4) for i in range(4)])


def across(x, dc, dz):
    pairs = [(c * 8 + z, (c ^ dc) * 8 + (z ^ dz)) for c in range(2) for z in range(8)]
    return lax.ppermute(x, ("c", "z"), pairs)


def on_device(queries, keys, values, log_forget, strength, out_weight):
    front = lax.axis_index("c") == 0
    rows = jnp.stack((queries, keys, values))
    gates = jnp.stack((log_forget, strength), axis=1)
    keep = jnp.where(front, rows[:, :, 0], rows[:, :, 1])
    send = jnp.where(front, rows[:, :, 1], rows[:, :, 0])
    gate_keep = jnp.where(front, gates[0], gates[1])
    gate_send = jnp.where(front, gates[1], gates[0])
    received = across(send, 1, 0)
    gate_received = across(gate_send, 1, 0)
    pair_weight = across(out_weight, 0, 1)
    q, kv, gates, local, first = call(
        gram_body,
        [
            ((CHIP, E), bf16),
            ((2, CHIP, E), bf16),
            ((8, HALF), f32),
            ((ROWS, E), bf16),
            ((2 * E, E), f32),
        ],
        [],
        1 << 26,
        keep,
        received,
        gate_keep,
        gate_received,
    )
    around_y = [turned(local, "y", by) for by in (1, 2, 3)]
    halos = [beyond(kv, 1), beyond(kv, 2)]
    row_total, state, lead = call(
        row_body,
        [((ROWS, E), bf16), ((ROWS, E), f32), ((8, E), f32)],
        [((4, ROWS, E), bf16)],
        1 << 20,
        local,
        *around_y,
    )
    around_x = [turned(row_total, "x", by) for by in (1, 2, 3)]
    prepared = call(
        prepare_body,
        [
            ((2, HALF, HALF), f32),
            ((2, HALF, HALF), f32),
            ((2, E, HALF), bf16),
            ((2, E, HALF), bf16),
            ((2, E, HALF), f32),
            ((8, HALF), f32),
        ],
        [],
        1 << 26,
        q,
        kv,
        gates,
    )
    (mesa,) = call(
        solve_body,
        [((E, CHIP), f32)],
        [
            ((2, CHIP, 2 * E), bf16),
        ],
        1 << 30,
        kv,
        gates,
        first,
        state,
        lead,
        *prepared,
        *around_x,
    )
    kept, to_c, to_z, to_cz = call(
        attend_body,
        [((HALF // 2, E), bf16)] * 4,
        [((2 * SLOTS, SLOT, E), bf16)],
        1 << 29,
        q,
        kv,
        *halos,
        mesa,
    )
    from_cz = across(to_cz, 1, 1)
    from_z = across(to_z, 0, 1)
    from_c = across(to_c, 1, 0)
    mine, *sent = call(
        project_body,
        [((SLOT, 2048), f32)] + [((SLOT, 2048), bf16)] * 3,
        [((HALF // 2, 4 * E), bf16)],
        1 << 28,
        kept,
        from_c,
        from_z,
        from_cz,
        out_weight,
        pair_weight,
    )
    got = []
    for away, share in reversed(list(enumerate(sent, 1))):
        pairs = [(z, (z + (2 * (z % 2) - 1) * away) % SLOTS) for z in range(SLOTS)]
        got.append(lax.ppermute(share, "z", pairs))
    (total,) = call(sum_body, [((SLOT, 2048), bf16)], [], 1 << 18, mine, *got)
    return total


def solution(mesh):
    grid = Mesh(mesh.devices.reshape(4, 4, 2, mesh.shape["head"]), ("x", "y", "c", "z"))
    in_specs = (
        P(SEQ, "z", None),
        P(SEQ, "z", None),
        P(SEQ, "z", None),
        P("z", SEQ),
        P("z", SEQ),
        P("z", None),
    )

    return jax.shard_map(
        on_device, mesh=grid, in_specs=in_specs, out_specs=P((*SEQ, "z"), None), check_vma=False
    )
```

```python
import jax
import jax.numpy as jnp
from jax import lax
from jax.experimental import pallas as pl
from jax.experimental.pallas import tpu as pltpu
from jax.sharding import Mesh
from jax.sharding import PartitionSpec as P

CG_STEPS = 6
RIDGE = 0.25
TINY = 1e-30
LOW = -1e30
HALF = 256
E = 128
CHIP = 2 * HALF
SIDE = E // 2
BODY = SIDE + E
ROWS = BODY + 16
SLOT = 32
SLOTS = 8
GRANT = 16 << 20
SEQ = ("x", "y", "c")
XY = ("x", "y")
f32 = jnp.float32
bf16 = jnp.bfloat16


def spec(kind=pltpu.VMEM):
    return pl.BlockSpec(memory_space=kind)


def call(body, outs, scratch, flops, *args):
    return pl.pallas_call(
        body,
        out_shape=[jax.ShapeDtypeStruct(shape, kind) for shape, kind in outs],
        in_specs=[spec()] * len(args),
        out_specs=[spec()] * len(outs),
        scratch_shapes=[pltpu.VMEM(shape, kind) for shape, kind in scratch],
        compiler_params=pltpu.CompilerParams(vmem_limit_bytes=GRANT),
        cost_estimate=pl.CostEstimate(flops=flops, bytes_accessed=1 << 20, transcendentals=0),
    )(*args)


def split(x):
    high = x.astype(bf16)
    return high, (x - high.astype(f32)).astype(bf16)


def dot(a, b):
    return jnp.dot(a, b, preferred_element_type=f32)


def two_part(a, b):
    high, low = split(b)
    return dot(a, high) + dot(a, low)


def iotas(shape):
    return lax.broadcasted_iota(jnp.int32, shape, 0), lax.broadcasted_iota(jnp.int32, shape, 1)


def packed(state):
    top, bottom = state[:SIDE], pltpu.roll(state[SIDE:E], SIDE, 1)
    row, col = iotas((SIDE, E))
    square = jnp.where((col < SIDE) & (row < col), bottom, top)
    diagonal = jnp.sum(jnp.where(row == col, bottom, 0.0), axis=0, keepdims=True)
    line, _ = iotas((16, E))
    return jnp.concatenate((square, state[E:], jnp.where(line == 2, diagonal, 0.0)), axis=0)


def unpacked(state):
    square, diagonal = state[:SIDE], state[BODY + 2 : BODY + 3]
    turned_square = jnp.transpose(jnp.concatenate((square, jnp.zeros((SIDE, E), f32)), axis=0))
    other = turned_square[:SIDE]
    row, col = iotas((SIDE, E))
    top = jnp.where((col < SIDE) & (row < col), other, square)
    corner = jnp.where(row < col, square, jnp.where(row > col, other, diagonal))
    bottom = jnp.where(col < SIDE, turned_square[SIDE:], pltpu.roll(corner, SIDE, 1))
    return jnp.concatenate((top, bottom, state[SIDE:BODY]), axis=0)


def payload(state, total):
    high, low = split(total)
    row, _ = iotas((16, E))
    tail = jnp.where(
        row == 0, high.astype(f32), jnp.where(row == 1, low.astype(f32), state[BODY:])
    )
    return jnp.concatenate((state[:BODY], tail), axis=0).astype(bf16)


def decay_row(tail):
    wide = tail.astype(f32)
    return wide[0:1, :] + wide[1:2, :]


def gram_body(keep, recv, gate_keep, gate_recv, q_out, kv_out, gates_out, pay_out, first_out):
    core = lax.axis_index("c")
    for source, which in ((keep, core), (recv, 1 - core)):
        rows = pl.ds(pl.multiple_of(which * HALF, HALF), HALF)
        q_out[rows, :] = source[0]
        kv_out[0, rows, :] = source[1]
        kv_out[1, rows, :] = source[2]
    a, b = gate_keep[...], gate_recv[...]
    first, second = jnp.where(core == 0, a, b), jnp.where(core == 0, b, a)
    forget = jnp.concatenate((first[0:1], second[0:1], jnp.zeros((6, HALF), f32)), axis=0)
    row, col = iotas((HALF, HALF))
    upto = (row <= col).astype(f32)
    sums = jnp.dot(forget, upto, preferred_element_type=f32, precision=lax.Precision.HIGHEST)
    gates_out[...] = jnp.concatenate(
        (sums[0:2], first[1:2], second[1:2], jnp.zeros((4, HALF), f32)), axis=0
    )
    grams = []
    for j in range(2):
        own = slice(j * HALF, (j + 1) * HALF)
        k = kv_out[0, own, :]
        kt = jnp.transpose(k.astype(f32))
        vt = jnp.transpose(kv_out[1, own, :].astype(f32))
        r = lax.rsqrt(jnp.sum(kt * kt, axis=0, keepdims=True) + 1e-6)
        weight = jnp.exp(sums[j : j + 1, HALF - 1 :] - sums[j : j + 1]) * gates_out[2 + j : 3 + j]
        left = jnp.concatenate((kt * (weight * r * r), vt * (weight * r)), axis=0)
        high, low = split(left)
        grams.append(dot(high, k) + dot(low, k))
    first_out[...] = grams[0]
    later = sums[1:2, HALF - 1 :]
    local = jnp.exp(later) * grams[0] + grams[1]
    pay_out[...] = payload(packed(local), jnp.broadcast_to(sums[0:1, HALF - 1 :] + later, (1, E)))


def row_body(own, r1, r2, r3, pay_out, state_out, lead_out, place):
    mine = lax.axis_index("y")
    place[mine] = own[...]
    for distance, received in ((1, r1), (2, r2), (3, r3)):
        place[lax.rem(mine + 4 - distance, 4)] = received[...]
    decays = [decay_row(place[m, BODY:, :]) for m in range(4)]
    zero = jnp.zeros((1, E), f32)
    total = before = jnp.zeros((ROWS, E), f32)
    lead = zero
    for m in range(4):
        block = place[m].astype(f32)
        step = jnp.exp(decays[m])
        total = step * total + block
        earlier = m < mine
        before = jnp.where(earlier, step * before + block, before)
        lead = jnp.where(earlier, lead + decays[m], lead)
    pay_out[...] = payload(total, decays[0] + decays[1] + decays[2] + decays[3])
    state_out[...] = before
    lead_out[...] = jnp.broadcast_to(lead, (8, E))


def prepare_body(q, kv, gates, mix, mix_v, keys_t, values_t, queries_t, leads):
    row, col = iotas((HALF, HALF))
    causal = row <= col
    line_of, _ = iotas((E, HALF))
    for j in range(2):
        own = slice(j * HALF, (j + 1) * HALF)
        kt = jnp.transpose(kv[0, own, :].astype(f32))
        keys_t[j] = kt.astype(bf16)
        values_t[j] = jnp.transpose(kv[1, own, :].astype(f32)).astype(bf16)
        r = lax.rsqrt(jnp.sum(kt * kt, axis=0, keepdims=True) + 1e-6)
        c = gates[j : j + 1, :]
        strength = gates[2 + j : 3 + j, :]
        columns = jnp.transpose(
            jnp.where(
                line_of == 0, c, jnp.where(line_of == 1, strength * r * r, strength * r)
            )
        )
        gap = jnp.where(causal, c - columns[:, 0:1], 0.0)
        decay = jnp.where(causal, jnp.exp(gap), 0.0)
        mix[j] = decay * columns[:, 1:2]
        mix_v[j] = decay * columns[:, 2:3]
        qt = jnp.transpose(q[own, :].astype(f32))
        queries_t[j] = qt * lax.rsqrt(jnp.sum(qt * qt, axis=0, keepdims=True) + 1e-6)
    leads[...] = jnp.exp(gates[...])


def place_state(left, j, state):
    high, low = split(state)
    left[j, HALF : HALF + E, :E] = high
    left[j, HALF : HALF + E, E:] = high
    left[j, HALF + E :, :E] = low
    left[j, HALF + E :, E:] = jnp.zeros((E, E), bf16)


def solve_body(
    kv, gates, first, state, lead, mix, mix_v, keys_t, values_t, queries_t, leads, t1, t2, t3,
    out, left,
):
    line = lax.axis_index("x")
    start = jnp.zeros((ROWS, E), f32)
    passed = jnp.zeros((1, E), f32)
    for distance, received in ((1, t1), (2, t2), (3, t3)):
        block = received[...].astype(f32)
        start = jnp.where(line >= distance, start + jnp.exp(passed) * block, start)
        passed = passed + decay_row(received[BODY:, :])
    start = unpacked(jnp.exp(lead[0:1, :]) * start + state[...])
    starts = [start, jnp.exp(gates[0:1, HALF - 1 :]) * start + first[...]]
    for j in range(2):
        k = kv[0, j * HALF : (j + 1) * HALF, :]
        left[j, :HALF, :E] = k
        left[j, :HALF, E:] = k
        place_state(left, j, starts[j][:E])

    def products(j, vector, weights, right):
        high, low = split(vector)
        y = dot(left[j], jnp.concatenate((high, low), axis=0))
        inside = two_part(right, weights * y[:HALF])
        return leads[j : j + 1, :] * (y[HALF : HALF + E] + y[HALF + E :]) + inside

    xs = [jnp.zeros((E, HALF), f32)] * 2
    rs = [queries_t[j] for j in range(2)]
    ds = list(rs)
    norms = [jnp.sum(r * r, axis=0, keepdims=True) for r in rs]
    for _ in range(CG_STEPS):
        for j in range(2):
            d = ds[j]
            image = products(j, d, mix[j], keys_t[j]) + RIDGE * d
            alpha = norms[j] / jnp.maximum(jnp.sum(d * image, axis=0, keepdims=True), TINY)
            xs[j] = xs[j] + alpha * d
            rs[j] = rs[j] - alpha * image
            new = jnp.sum(rs[j] * rs[j], axis=0, keepdims=True)
            ds[j] = rs[j] + new / jnp.maximum(norms[j], TINY) * d
            norms[j] = new
    for j in range(2):
        place_state(left, j, starts[j][E:])
        out[:, j * HALF : (j + 1) * HALF] = products(j, xs[j], mix_v[j], values_t[j])


def products_of(parts, qj, largest, total, result):
    scale = E ** (-0.5)
    scores = []
    for keys, _, mask in parts:
        s = lax.dot_general(keys, qj, (((1,), (1,)), ((), ())), preferred_element_type=f32)
        scores.append(s if mask is None else jnp.where(mask, s, LOW))
    top = scores[0]
    for s in scores[1:]:
        top = jnp.maximum(top, s)
    top = jnp.max(top, axis=0, keepdims=True)
    if largest is not None:
        top = jnp.maximum(top, largest)
        shrink = jnp.exp((largest - top) * scale)
        total, result = total * shrink, result * shrink
    for (_, values_t, _), s in zip(parts, scores):
        expo = jnp.exp((s - top) * scale)
        total = total + jnp.sum(expo, axis=0, keepdims=True)
        result = result + dot(values_t, expo.astype(bf16))
    return top, total, result


def blocks_of(source):
    rows = [slice(half * HALF, (half + 1) * HALF) for half in range(2)]
    return [(source[0, r, :], jnp.transpose(source[1, r, :].astype(f32)).astype(bf16)) for r in rows]


def attend_a_body(q, kv, far, rows_out, result_out):
    chip = lax.axis_index("x") * 4 + lax.axis_index("y")
    row, col = iotas((HALF, HALF))
    old, own = blocks_of(far), blocks_of(kv)
    held = chip >= 2
    lines = []
    for j in range(2):
        parts = [(*old[j], (row > col) & held)]
        if j == 0:
            parts.append((*old[1], held))
        else:
            parts.append((*own[0], None))
        parts.append((*own[j], row <= col))
        at = slice(j * HALF, (j + 1) * HALF)
        top, total, result = products_of(
            parts, q[at, :], None, jnp.zeros((1, HALF), f32), jnp.zeros((E, HALF), f32)
        )
        lines += [top, total]
        result_out[:, at] = result
    rows_out[...] = jnp.concatenate((*lines, jnp.zeros((4, HALF), f32)), axis=0)


def attend_body(q, near, rows, first, mesa, keep_out, c_out, z_out, cz_out, place):
    core = lax.axis_index("c")
    held = lax.axis_index("x") * 4 + lax.axis_index("y") >= 1
    parts = [(*block, held) for block in blocks_of(near)]
    for j in range(2):
        at = slice(j * HALF, (j + 1) * HALF)
        top, total = rows[2 * j : 2 * j + 1, :], rows[2 * j + 1 : 2 * j + 2, :]
        _, total, result = products_of(parts, q[at, :], top, total, first[:, at])
        both = jnp.transpose(result / total + mesa[:, at]).astype(bf16)
        for slot in range(SLOTS):
            place[SLOTS * j + slot] = both[slot * SLOT : (slot + 1) * SLOT]

    def piece(which, device):
        way = 2 * lax.rem(device, 2) - 1
        return jnp.concatenate(
            [
                place[SLOTS * which + lax.rem(device + way * away + SLOTS, SLOTS)]
                for away in range(SLOTS // 2)
            ],
            axis=0,
        )

    here = lax.axis_index("z")
    there = here + 1 - 2 * lax.rem(here, 2)
    keep_out[...] = piece(core, here)
    c_out[...] = piece(1 - core, here)
    z_out[...] = piece(core, there)
    cz_out[...] = piece(1 - core, there)


def project_body(keep, from_c, from_z, from_cz, own_weight, pair_weight, mine, s1, s2, s3, wide):
    core = lax.axis_index("c")
    for piece, at in (
        (keep, core),
        (from_c, 1 - core),
        (from_z, 2 + core),
        (from_cz, 3 - core),
    ):
        wide[:, pl.ds(pl.multiple_of(at * E, E), E)] = piece[...]
    y = dot(wide[:, : 2 * E], own_weight[...]) + dot(wide[:, 2 * E :], pair_weight[...])
    mine[...] = y[:SLOT]
    for d, out in ((1, s1), (2, s2), (3, s3)):
        out[...] = y[d * SLOT : (d + 1) * SLOT].astype(bf16)


def sum_body(mine, a, b, c, out):
    out[...] = (mine[...] + a[...].astype(f32) + b[...].astype(f32) + c[...].astype(f32)).astype(
        bf16
    )


def beyond(x, by):
    return lax.ppermute(x, XY, [(i, (i + by) % 16) for i in range(16)])


def turned(x, axis, by):
    return lax.ppermute(x, axis, [(i, (i + by) % 4) for i in range(4)])


def across(x, dc, dz):
    pairs = [(c * 8 + z, (c ^ dc) * 8 + (z ^ dz)) for c in range(2) for z in range(8)]
    return lax.ppermute(x, ("c", "z"), pairs)


def on_device(queries, keys, values, log_forget, strength, out_weight):
    front = lax.axis_index("c") == 0
    rows = jnp.stack((queries, keys, values))
    gates = jnp.stack((log_forget, strength), axis=1)
    keep = jnp.where(front, rows[:, :, 0], rows[:, :, 1])
    send = jnp.where(front, rows[:, :, 1], rows[:, :, 0])
    gate_keep = jnp.where(front, gates[0], gates[1])
    gate_send = jnp.where(front, gates[1], gates[0])
    received = across(send, 1, 0)
    gate_received = across(gate_send, 1, 0)
    pair_weight = across(out_weight, 0, 1)
    q, kv, gates, local, first = call(
        gram_body,
        [
            ((CHIP, E), bf16),
            ((2, CHIP, E), bf16),
            ((8, HALF), f32),
            ((ROWS, E), bf16),
            ((2 * E, E), f32),
        ],
        [],
        1 << 26,
        keep,
        received,
        gate_keep,
        gate_received,
    )
    around_y = [turned(local, "y", by) for by in (1, 2, 3)]
    halos = [beyond(kv, 1), beyond(kv, 2)]
    row_total, state, lead = call(
        row_body,
        [((ROWS, E), bf16), ((ROWS, E), f32), ((8, E), f32)],
        [((4, ROWS, E), bf16)],
        1 << 20,
        local,
        *around_y,
    )
    around_x = [turned(row_total, "x", by) for by in (1, 2, 3)]
    prepared = call(
        prepare_body,
        [
            ((2, HALF, HALF), f32),
            ((2, HALF, HALF), f32),
            ((2, E, HALF), bf16),
            ((2, E, HALF), bf16),
            ((2, E, HALF), f32),
            ((8, HALF), f32),
        ],
        [],
        1 << 26,
        q,
        kv,
        gates,
    )
    (mesa,) = call(
        solve_body,
        [((E, CHIP), f32)],
        [
            ((2, CHIP, 2 * E), bf16),
        ],
        1 << 30,
        kv,
        gates,
        first,
        state,
        lead,
        *prepared,
        *around_x,
    )
    near, far = halos
    partial = call(attend_a_body, [((8, HALF), f32), ((E, CHIP), f32)], [], 1 << 28, q, kv, far)
    kept, to_c, to_z, to_cz = call(
        attend_body,
        [((HALF // 2, E), bf16)] * 4,
        [((2 * SLOTS, SLOT, E), bf16)],
        1 << 29,
        q,
        near,
        *partial,
        mesa,
    )
    from_cz = across(to_cz, 1, 1)
    from_z = across(to_z, 0, 1)
    from_c = across(to_c, 1, 0)
    mine, *sent = call(
        project_body,
        [((SLOT, 2048), f32)] + [((SLOT, 2048), bf16)] * 3,
        [((HALF // 2, 4 * E), bf16)],
        1 << 28,
        kept,
        from_c,
        from_z,
        from_cz,
        out_weight,
        pair_weight,
    )
    got = []
    for away, share in reversed(list(enumerate(sent, 1))):
        pairs = [(z, (z + (2 * (z % 2) - 1) * away) % SLOTS) for z in range(SLOTS)]
        got.append(lax.ppermute(share, "z", pairs))
    (total,) = call(sum_body, [((SLOT, 2048), bf16)], [], 1 << 18, mine, *got)
    return total


def solution(mesh):
    grid = Mesh(mesh.devices.reshape(4, 4, 2, mesh.shape["head"]), ("x", "y", "c", "z"))
    in_specs = (
        P(SEQ, "z", None),
        P(SEQ, "z", None),
        P(SEQ, "z", None),
        P("z", SEQ),
        P("z", SEQ),
        P("z", None),
    )

    return jax.shard_map(
        on_device, mesh=grid, in_specs=in_specs, out_specs=P((*SEQ, "z"), None), check_vma=False
    )
```

```python
import jax
import jax.numpy as jnp
from jax import lax
from jax.experimental import pallas as pl
from jax.experimental.pallas import tpu as pltpu
from jax.sharding import Mesh
from jax.sharding import PartitionSpec as P

CG_STEPS = 6
RIDGE = 0.25
TINY = 1e-30
LOW = -1e30
HALF = 256
E = 128
CHIP = 2 * HALF
SIDE = E // 2
BODY = SIDE + E
ROWS = BODY + 16
SLOT = 32
SLOTS = 8
GRANT = 16 << 20
SEQ = ("x", "y", "c")
XY = ("x", "y")
f32 = jnp.float32
bf16 = jnp.bfloat16


def spec(kind=pltpu.VMEM):
    return pl.BlockSpec(memory_space=kind)


def call(body, outs, scratch, flops, *args):
    return pl.pallas_call(
        body,
        out_shape=[jax.ShapeDtypeStruct(shape, kind) for shape, kind in outs],
        in_specs=[spec()] * len(args),
        out_specs=[spec()] * len(outs),
        scratch_shapes=[pltpu.VMEM(shape, kind) for shape, kind in scratch],
        compiler_params=pltpu.CompilerParams(vmem_limit_bytes=GRANT),
        cost_estimate=pl.CostEstimate(flops=flops, bytes_accessed=1 << 20, transcendentals=0),
    )(*args)


def split(x):
    high = x.astype(bf16)
    return high, (x - high.astype(f32)).astype(bf16)


def dot(a, b):
    return jnp.dot(a, b, preferred_element_type=f32)


def two_part(a, b):
    high, low = split(b)
    return dot(a, high) + dot(a, low)


def iotas(shape):
    return lax.broadcasted_iota(jnp.int32, shape, 0), lax.broadcasted_iota(jnp.int32, shape, 1)


def packed(state):
    top, bottom = state[:SIDE], pltpu.roll(state[SIDE:E], SIDE, 1)
    row, col = iotas((SIDE, E))
    square = jnp.where((col < SIDE) & (row < col), bottom, top)
    diagonal = jnp.sum(jnp.where(row == col, bottom, 0.0), axis=0, keepdims=True)
    line, _ = iotas((16, E))
    return jnp.concatenate((square, state[E:], jnp.where(line == 2, diagonal, 0.0)), axis=0)


def unpacked(state):
    square, diagonal = state[:SIDE], state[BODY + 2 : BODY + 3]
    turned_square = jnp.transpose(jnp.concatenate((square, jnp.zeros((SIDE, E), f32)), axis=0))
    other = turned_square[:SIDE]
    row, col = iotas((SIDE, E))
    top = jnp.where((col < SIDE) & (row < col), other, square)
    corner = jnp.where(row < col, square, jnp.where(row > col, other, diagonal))
    bottom = jnp.where(col < SIDE, turned_square[SIDE:], pltpu.roll(corner, SIDE, 1))
    return jnp.concatenate((top, bottom, state[SIDE:BODY]), axis=0)


def payload(state, total):
    high, low = split(total)
    row, _ = iotas((16, E))
    tail = jnp.where(
        row == 0, high.astype(f32), jnp.where(row == 1, low.astype(f32), state[BODY:])
    )
    return jnp.concatenate((state[:BODY], tail), axis=0).astype(bf16)


def decay_row(tail):
    wide = tail.astype(f32)
    return wide[0:1, :] + wide[1:2, :]


def gram_body(keep, recv, gate_keep, gate_recv, q_out, kv_out, gates_out, pay_out, first_out):
    core = lax.axis_index("c")
    for source, which in ((keep, core), (recv, 1 - core)):
        rows = pl.ds(pl.multiple_of(which * HALF, HALF), HALF)
        q_out[rows, :] = source[0]
        kv_out[0, rows, :] = source[1]
        kv_out[1, rows, :] = source[2]
    a, b = gate_keep[...], gate_recv[...]
    first, second = jnp.where(core == 0, a, b), jnp.where(core == 0, b, a)
    forget = jnp.concatenate((first[0:1], second[0:1], jnp.zeros((6, HALF), f32)), axis=0)
    row, col = iotas((HALF, HALF))
    upto = (row <= col).astype(f32)
    sums = jnp.dot(forget, upto, preferred_element_type=f32, precision=lax.Precision.HIGHEST)
    gates_out[...] = jnp.concatenate(
        (sums[0:2], first[1:2], second[1:2], jnp.zeros((4, HALF), f32)), axis=0
    )
    grams = []
    for j in range(2):
        own = slice(j * HALF, (j + 1) * HALF)
        k = kv_out[0, own, :]
        kt = jnp.transpose(k.astype(f32))
        vt = jnp.transpose(kv_out[1, own, :].astype(f32))
        r = lax.rsqrt(jnp.sum(kt * kt, axis=0, keepdims=True) + 1e-6)
        weight = jnp.exp(sums[j : j + 1, HALF - 1 :] - sums[j : j + 1]) * gates_out[2 + j : 3 + j]
        left = jnp.concatenate((kt * (weight * r * r), vt * (weight * r)), axis=0)
        high, low = split(left)
        grams.append(dot(high, k) + dot(low, k))
    first_out[...] = grams[0]
    later = sums[1:2, HALF - 1 :]
    local = jnp.exp(later) * grams[0] + grams[1]
    pay_out[...] = payload(packed(local), jnp.broadcast_to(sums[0:1, HALF - 1 :] + later, (1, E)))


def row_body(own, r1, r2, r3, pay_out, state_out, lead_out, place):
    mine = lax.axis_index("y")
    place[mine] = own[...]
    for distance, received in ((1, r1), (2, r2), (3, r3)):
        place[lax.rem(mine + 4 - distance, 4)] = received[...]
    decays = [decay_row(place[m, BODY:, :]) for m in range(4)]
    zero = jnp.zeros((1, E), f32)
    total = before = jnp.zeros((ROWS, E), f32)
    lead = zero
    for m in range(4):
        block = place[m].astype(f32)
        step = jnp.exp(decays[m])
        total = step * total + block
        earlier = m < mine
        before = jnp.where(earlier, step * before + block, before)
        lead = jnp.where(earlier, lead + decays[m], lead)
    pay_out[...] = payload(total, decays[0] + decays[1] + decays[2] + decays[3])
    state_out[...] = before
    lead_out[...] = jnp.broadcast_to(lead, (8, E))


def prepare_body(q, kv, gates, mix, mix_v, keys_t, values_t, queries_t, leads):
    row, col = iotas((HALF, HALF))
    causal = row <= col
    line_of, _ = iotas((E, HALF))
    for j in range(2):
        own = slice(j * HALF, (j + 1) * HALF)
        kt = jnp.transpose(kv[0, own, :].astype(f32))
        keys_t[j] = kt.astype(bf16)
        values_t[j] = jnp.transpose(kv[1, own, :].astype(f32)).astype(bf16)
        r = lax.rsqrt(jnp.sum(kt * kt, axis=0, keepdims=True) + 1e-6)
        c = gates[j : j + 1, :]
        strength = gates[2 + j : 3 + j, :]
        columns = jnp.transpose(
            jnp.where(
                line_of == 0, c, jnp.where(line_of == 1, strength * r * r, strength * r)
            )
        )
        gap = jnp.where(causal, c - columns[:, 0:1], 0.0)
        decay = jnp.where(causal, jnp.exp(gap), 0.0)
        mix[j] = decay * columns[:, 1:2]
        mix_v[j] = decay * columns[:, 2:3]
        qt = jnp.transpose(q[own, :].astype(f32))
        queries_t[j] = qt * lax.rsqrt(jnp.sum(qt * qt, axis=0, keepdims=True) + 1e-6)
    leads[...] = jnp.exp(gates[...])


def place_state(left, j, state):
    high, low = split(state)
    left[j, HALF : HALF + E, :E] = high
    left[j, HALF : HALF + E, E:] = high
    left[j, HALF + E :, :E] = low
    left[j, HALF + E :, E:] = jnp.zeros((E, E), bf16)


def solve_body(
    kv, gates, first, state, lead, mix, mix_v, keys_t, values_t, queries_t, leads, t1, t2, t3,
    out, left,
):
    line = lax.axis_index("x")
    start = jnp.zeros((ROWS, E), f32)
    passed = jnp.zeros((1, E), f32)
    for distance, received in ((1, t1), (2, t2), (3, t3)):
        block = received[...].astype(f32)
        start = jnp.where(line >= distance, start + jnp.exp(passed) * block, start)
        passed = passed + decay_row(received[BODY:, :])
    start = unpacked(jnp.exp(lead[0:1, :]) * start + state[...])
    starts = [start, jnp.exp(gates[0:1, HALF - 1 :]) * start + first[...]]
    for j in range(2):
        k = kv[0, j * HALF : (j + 1) * HALF, :]
        left[j, :HALF, :E] = k
        left[j, :HALF, E:] = k
        place_state(left, j, starts[j][:E])

    def products(j, vector, weights, right):
        high, low = split(vector)
        y = dot(left[j], jnp.concatenate((high, low), axis=0))
        inside = two_part(right, weights * y[:HALF])
        return leads[j : j + 1, :] * (y[HALF : HALF + E] + y[HALF + E :]) + inside

    xs = [jnp.zeros((E, HALF), f32)] * 2
    rs = [queries_t[j] for j in range(2)]
    ds = list(rs)
    norms = [jnp.sum(r * r, axis=0, keepdims=True) for r in rs]
    for _ in range(CG_STEPS):
        for j in range(2):
            d = ds[j]
            image = products(j, d, mix[j], keys_t[j]) + RIDGE * d
            alpha = norms[j] / jnp.maximum(jnp.sum(d * image, axis=0, keepdims=True), TINY)
            xs[j] = xs[j] + alpha * d
            rs[j] = rs[j] - alpha * image
            new = jnp.sum(rs[j] * rs[j], axis=0, keepdims=True)
            ds[j] = rs[j] + new / jnp.maximum(norms[j], TINY) * d
            norms[j] = new
    for j in range(2):
        place_state(left, j, starts[j][E:])
        out[:, j * HALF : (j + 1) * HALF] = products(j, xs[j], mix_v[j], values_t[j])


def products_of(parts, qj, largest, total, result):
    scale = E ** (-0.5)
    scores = []
    for keys, _, mask in parts:
        s = lax.dot_general(keys, qj, (((1,), (1,)), ((), ())), preferred_element_type=f32)
        scores.append(s if mask is None else jnp.where(mask, s, LOW))
    top = scores[0]
    for s in scores[1:]:
        top = jnp.maximum(top, s)
    top = jnp.max(top, axis=0, keepdims=True)
    if largest is not None:
        top = jnp.maximum(top, largest)
        shrink = jnp.exp((largest - top) * scale)
        total, result = total * shrink, result * shrink
    for (_, values_t, _), s in zip(parts, scores):
        expo = jnp.exp((s - top) * scale)
        total = total + jnp.sum(expo, axis=0, keepdims=True)
        result = result + dot(values_t, expo.astype(bf16))
    return top, total, result


def blocks_of(source):
    rows = [slice(half * HALF, (half + 1) * HALF) for half in range(2)]
    return [(source[0, r, :], jnp.transpose(source[1, r, :].astype(f32)).astype(bf16)) for r in rows]


def store_partial(rows_out, result_out, found):
    lines = []
    for j, (top, total, result) in enumerate(found):
        lines += [top, total]
        result_out[:, j * HALF : (j + 1) * HALF] = result
    rows_out[...] = jnp.concatenate((*lines, jnp.zeros((4, HALF), f32)), axis=0)


def attend_own_body(q, kv, rows_out, result_out):
    row, col = iotas((HALF, HALF))
    own, found = blocks_of(kv), []
    for j in range(2):
        parts = [(*own[0], None)] * j + [(*own[j], row <= col)]
        start = None, jnp.zeros((1, HALF), f32), jnp.zeros((E, HALF), f32)
        found.append(products_of(parts, q[j * HALF : (j + 1) * HALF, :], *start))
    store_partial(rows_out, result_out, found)


def attend_a_body(q, far, rows, first, rows_out, result_out):
    held = lax.axis_index("x") * 4 + lax.axis_index("y") >= 2
    row, col = iotas((HALF, HALF))
    old, found = blocks_of(far), []
    for j in range(2):
        at = slice(j * HALF, (j + 1) * HALF)
        parts = [(*old[j], (row > col) & held)] + [(*old[1], held)] * (1 - j)
        top, total = rows[2 * j : 2 * j + 1, :], rows[2 * j + 1 : 2 * j + 2, :]
        found.append(products_of(parts, q[at, :], top, total, first[:, at]))
    store_partial(rows_out, result_out, found)


def attend_body(q, near, rows, first, mesa, keep_out, c_out, z_out, cz_out, place):
    core = lax.axis_index("c")
    held = lax.axis_index("x") * 4 + lax.axis_index("y") >= 1
    parts = [(*block, held) for block in blocks_of(near)]
    for j in range(2):
        at = slice(j * HALF, (j + 1) * HALF)
        top, total = rows[2 * j : 2 * j + 1, :], rows[2 * j + 1 : 2 * j + 2, :]
        _, total, result = products_of(parts, q[at, :], top, total, first[:, at])
        both = jnp.transpose(result / total + mesa[:, at]).astype(bf16)
        for slot in range(SLOTS):
            place[SLOTS * j + slot] = both[slot * SLOT : (slot + 1) * SLOT]

    def piece(which, device):
        way = 2 * lax.rem(device, 2) - 1
        return jnp.concatenate(
            [
                place[SLOTS * which + lax.rem(device + way * away + SLOTS, SLOTS)]
                for away in range(SLOTS // 2)
            ],
            axis=0,
        )

    here = lax.axis_index("z")
    there = here + 1 - 2 * lax.rem(here, 2)
    keep_out[...] = piece(core, here)
    c_out[...] = piece(1 - core, here)
    z_out[...] = piece(core, there)
    cz_out[...] = piece(1 - core, there)


def project_body(keep, from_c, from_z, from_cz, own_weight, pair_weight, mine, s1, s2, s3, wide):
    core = lax.axis_index("c")
    for piece, at in (
        (keep, core),
        (from_c, 1 - core),
        (from_z, 2 + core),
        (from_cz, 3 - core),
    ):
        wide[:, pl.ds(pl.multiple_of(at * E, E), E)] = piece[...]
    y = dot(wide[:, : 2 * E], own_weight[...]) + dot(wide[:, 2 * E :], pair_weight[...])
    mine[...] = y[:SLOT]
    for d, out in ((1, s1), (2, s2), (3, s3)):
        out[...] = y[d * SLOT : (d + 1) * SLOT].astype(bf16)


def sum_body(mine, a, b, c, out):
    out[...] = (mine[...] + a[...].astype(f32) + b[...].astype(f32) + c[...].astype(f32)).astype(
        bf16
    )


def beyond(x, by):
    return lax.ppermute(x, XY, [(i, (i + by) % 16) for i in range(16)])


def turned(x, axis, by):
    return lax.ppermute(x, axis, [(i, (i + by) % 4) for i in range(4)])


def across(x, dc, dz):
    pairs = [(c * 8 + z, (c ^ dc) * 8 + (z ^ dz)) for c in range(2) for z in range(8)]
    return lax.ppermute(x, ("c", "z"), pairs)


def on_device(queries, keys, values, log_forget, strength, out_weight):
    front = lax.axis_index("c") == 0
    rows = jnp.stack((queries, keys, values))
    gates = jnp.stack((log_forget, strength), axis=1)
    keep = jnp.where(front, rows[:, :, 0], rows[:, :, 1])
    send = jnp.where(front, rows[:, :, 1], rows[:, :, 0])
    gate_keep = jnp.where(front, gates[0], gates[1])
    gate_send = jnp.where(front, gates[1], gates[0])
    received = across(send, 1, 0)
    gate_received = across(gate_send, 1, 0)
    pair_weight = across(out_weight, 0, 1)
    q, kv, gates, local, first = call(
        gram_body,
        [
            ((CHIP, E), bf16),
            ((2, CHIP, E), bf16),
            ((8, HALF), f32),
            ((ROWS, E), bf16),
            ((2 * E, E), f32),
        ],
        [],
        1 << 26,
        keep,
        received,
        gate_keep,
        gate_received,
    )
    around_y = [turned(local, "y", by) for by in (1, 2, 3)]
    halos = [beyond(kv, 1), beyond(kv, 2)]
    row_total, state, lead = call(
        row_body,
        [((ROWS, E), bf16), ((ROWS, E), f32), ((8, E), f32)],
        [((4, ROWS, E), bf16)],
        1 << 20,
        local,
        *around_y,
    )
    around_x = [turned(row_total, "x", by) for by in (1, 2, 3)]
    prepared = call(
        prepare_body,
        [
            ((2, HALF, HALF), f32),
            ((2, HALF, HALF), f32),
            ((2, E, HALF), bf16),
            ((2, E, HALF), bf16),
            ((2, E, HALF), f32),
            ((8, HALF), f32),
        ],
        [],
        1 << 26,
        q,
        kv,
        gates,
    )
    (mesa,) = call(
        solve_body,
        [((E, CHIP), f32)],
        [
            ((2, CHIP, 2 * E), bf16),
        ],
        1 << 30,
        kv,
        gates,
        first,
        state,
        lead,
        *prepared,
        *around_x,
    )
    near, far = halos
    partial = call(attend_own_body, [((8, HALF), f32), ((E, CHIP), f32)], [], 1 << 27, q, kv)
    partial = call(
        attend_a_body, [((8, HALF), f32), ((E, CHIP), f32)], [], 1 << 28, q, far, *partial
    )
    kept, to_c, to_z, to_cz = call(
        attend_body,
        [((HALF // 2, E), bf16)] * 4,
        [((2 * SLOTS, SLOT, E), bf16)],
        1 << 29,
        q,
        near,
        *partial,
        mesa,
    )
    from_cz = across(to_cz, 1, 1)
    from_z = across(to_z, 0, 1)
    from_c = across(to_c, 1, 0)
    mine, *sent = call(
        project_body,
        [((SLOT, 2048), f32)] + [((SLOT, 2048), bf16)] * 3,
        [((HALF // 2, 4 * E), bf16)],
        1 << 28,
        kept,
        from_c,
        from_z,
        from_cz,
        out_weight,
        pair_weight,
    )
    got = []
    for away, share in reversed(list(enumerate(sent, 1))):
        pairs = [(z, (z + (2 * (z % 2) - 1) * away) % SLOTS) for z in range(SLOTS)]
        got.append(lax.ppermute(share, "z", pairs))
    (total,) = call(sum_body, [((SLOT, 2048), bf16)], [], 1 << 18, mine, *got)
    return total


def solution(mesh):
    grid = Mesh(mesh.devices.reshape(4, 4, 2, mesh.shape["head"]), ("x", "y", "c", "z"))
    in_specs = (
        P(SEQ, "z", None),
        P(SEQ, "z", None),
        P(SEQ, "z", None),
        P("z", SEQ),
        P("z", SEQ),
        P("z", None),
    )

    return jax.shard_map(
        on_device, mesh=grid, in_specs=in_specs, out_specs=P((*SEQ, "z"), None), check_vma=False
    )
```
